128 devices in a mesh: row: 8 (over z, core), col: 16 (over x, y).
Axes of the slice: x: 4, y: 4, z: 4, core: 2. Of those that a mesh axis runs over, the one named last changes fastest.
Arguments:
- point_coords: float32 [4096, 3, 256], P(('row', 'col')), may hold values from 0 to 10
- fluid_force: float32 [4096, 3, 256], P(('row', 'col')), may hold values from -6 to 6
- tile_clusters: int32 [4096, 8], P(('row', 'col')), may hold values from 0 to 2047, as said below
- pu_level: int32 [4096, 8, 256], P(('row', 'col')), may hold values from 0 to 15
- node_coords: float32 [2048, 3, 512], P(('row', 'col')), may hold values from 0 to 10
- node_disp: float32 [2048, 3, 512], P(('row', 'col')), may hold values from -6 to 6
- inverse: float32 [2048, 512, 512], P(('row', 'col')), may hold values from -0.25 to 0.25
Outputs:
- point_disp: float32 [4096, 3, 256], P(('row', 'col'))
- node_force: float32 [2048, 3, 512], P(('row', 'col'))
The draws below stay inside these ranges and needn't reach their ends.
Inputs may be any that keep to these rules, and one draw needn't show every extreme that they name: `tile_clusters`: cluster c lives with rows c of the cluster arrays; tile t's k-th entry names a cluster intersecting it, possibly more than once in a tile. Among the 256 entries of one device's tiles, at most 8 name clusters of any one device (clusters d * 16 to d * 16 + 15).
All inputs are finite; a program needn't handle non-finite values.
Results may differ from the reference program's by a relative error of at most 0.0003.
Values sent between devices are 32-bit elements; how exact they have to be, the bound alone decides.
A program may use at most 128 MiB of HBM per device.

```python
import jax
import jax.numpy as jnp
from jax import lax

NODES = 512
TILE = 256
KMAX = 8
CAP = 8
CL_DEV = 16
TILE_DEV = 32
CLUSTERS = 2048
TILES = 4096
N_ROW = 8
N_COL = 16


def tile_ids(key):
    dev_total = N_ROW * N_COL
    slot_total = dev_total * CAP
    pair_total = TILE_DEV * KMAX
    heat_level = jax.random.randint(jax.random.fold_in(key, 1), (dev_total,), 0, 4)
    hot_owner = jax.random.randint(jax.random.fold_in(key, 2), (), 0, dev_total)
    owner_of = jnp.arange(slot_total) // CAP
    base_score = jax.random.randint(jax.random.fold_in(key, 3), (dev_total, slot_total), 0, 512)
    scores = base_score + heat_level[owner_of][None, :] * 512 + jnp.where(owner_of == hot_owner, 8192, 0)[None, :]
    breakers = jax.vmap(lambda sub: jax.random.permutation(sub, slot_total))(jax.random.split(jax.random.fold_in(key, 4), dev_total))
    scores = scores * slot_total + breakers
    unused, chosen = lax.top_k(scores, pair_total)
    shuffles = jax.vmap(lambda sub: jax.random.permutation(sub, pair_total))(jax.random.split(jax.random.fold_in(key, 5), dev_total))
    chosen = jnp.take_along_axis(chosen, shuffles, axis=1)
    local_id = jax.random.randint(jax.random.fold_in(key, 6), (dev_total, pair_total), 0, CL_DEV)
    cluster_ids = chosen // CAP * CL_DEV + local_id
    return cluster_ids.reshape(dev_total * TILE_DEV, KMAX).astype(jnp.int32)


def cluster_centres(key):
    return jax.random.uniform(jax.random.fold_in(key, 20), (CLUSTERS, 3), jnp.float32, 1.0, 9.0)


def draw_tile_clusters(key, part):
    return tile_ids(key)


def draw_node_coords(key, part):
    centre = cluster_centres(key)
    half_width = jnp.array([0.5, 0.5, 0.5], jnp.float32)
    spread = jax.random.uniform(jax.random.fold_in(key, 21), (CLUSTERS, 3, NODES), jnp.float32, -1.0, 1.0)
    return (centre[:, :, None] + spread * half_width[None, :, None]).astype(jnp.float32)


def draw_point_coords(key, part):
    cluster_ids = tile_ids(key)
    centre = cluster_centres(key)
    pick = jax.random.randint(jax.random.fold_in(key, 22), (TILES, TILE), 0, KMAX)
    nearest = jnp.take_along_axis(cluster_ids, pick, axis=1)
    base = jnp.transpose(centre[nearest], (0, 2, 1))
    half_width = jnp.array([0.75, 0.75, 0.75], jnp.float32)
    spread = jax.random.uniform(jax.random.fold_in(key, 23), (TILES, 3, TILE), jnp.float32, -1.0, 1.0)
    return (base + spread * half_width[None, :, None]).astype(jnp.float32)


def touch_ends(values, key, smallest, top_value):
    longest = values.shape.index(max(values.shape))
    spots = []
    for shift in (0, 1):
        where = [jax.random.randint(jax.random.fold_in(key, axis), (), 0, length) for axis, length in enumerate(values.shape)]
        where[longest] = (where[longest] + shift) % values.shape[longest]
        spots.append(tuple(where))
    return values.at[spots[0]].set(smallest).at[spots[1]].set(top_value)


def block_levels(own_key, shape, cuts, smallest, top_value):
    def one(position, parts):
        heights = jax.random.uniform(jax.random.fold_in(jax.random.fold_in(own_key, 6), position), (parts,), jnp.float32, smallest / len(cuts), top_value / len(cuts))
        return jnp.repeat(jnp.exp(heights), shape[position] // parts).reshape((-1,) + (1,) * (len(shape) - position - 1))

    loudness = one(*cuts[0])
    for cut in cuts[1:]:
        loudness = loudness * one(*cut)
    return loudness


def noise(rng, shape, deviation, limit, cuts=(), kind=jnp.bfloat16):
    drawn = deviation * jax.random.normal(rng, shape, jnp.float32)
    if cuts:
        drawn = drawn * block_levels(rng, shape, cuts, -0.22, 0.18)
    return jnp.clip(drawn, -limit, limit).astype(kind)


def setup_inputs(seed: int = 0) -> dict:
    splits = jax.random.split(jax.random.key(seed), 8)
    return {
        "point_coords": draw_point_coords(jax.random.fold_in(splits[7], 71), 0),
        "fluid_force": noise(splits[1], (TILES, 3, TILE), 1.0, 6.0, ((0, 128),), jnp.float32),
        "tile_clusters": draw_tile_clusters(jax.random.fold_in(splits[7], 71), 0),
        "pu_level": touch_ends(jax.random.randint(splits[3], (TILES, KMAX, TILE), 0, 16), jax.random.fold_in(splits[3], 1), 0, 15).astype(jnp.int32),
        "node_coords": draw_node_coords(jax.random.fold_in(splits[7], 71), 0),
        "node_disp": noise(splits[5], (CLUSTERS, 3, NODES), 1.0, 6.0, ((0, 128),), jnp.float32),
        "inverse": noise(splits[6], (CLUSTERS, NODES, NODES), NODES ** -0.5, 0.25, ((0, 128),), jnp.float32),
    }


def kernel(points, node_rows):
    offset = points[..., :, :, None] - node_rows[..., :, None, :]
    scaled = jnp.sqrt(lax.optimization_barrier(jnp.sum(offset * offset, axis=-3)))
    return jnp.maximum(1.0 - scaled, 0.0) ** 4 * (4.0 * scaled + 1.0)

def reference(point_coords, fluid_force, tile_clusters, pu_level, node_coords, node_disp, inverse):
    highest = lax.Precision.HIGHEST
    coeffs = jnp.einsum('cin,cnm->cim', node_disp, inverse, precision=highest)
    levels = pu_level.astype(jnp.float32) + 1.0
    weights = levels / lax.optimization_barrier(jnp.sum(levels, axis=1, keepdims=True))

    def per_tile(force_sum, bundle):
        cluster_ids, points, tile_force, weight = bundle
        kernel_vals = kernel(points[None], node_coords[cluster_ids])
        values = jnp.einsum('kpn,kin->kip', kernel_vals, coeffs[cluster_ids], precision=highest)
        shown_disp = lax.optimization_barrier(jnp.sum(weight[:, None, :] * values, axis=0))
        loads = weight[:, None, :] * tile_force[None]
        partial_value = jnp.einsum('kpn,kip->kin', kernel_vals, loads, precision=highest)
        return (force_sum.at[cluster_ids].add(partial_value), shown_disp)
    empty_sum = jnp.zeros(node_coords.shape, jnp.float32)
    node_force, point_disp = lax.scan(per_tile, empty_sum, (tile_clusters, point_coords, fluid_force, weights))
    return (point_disp, node_force)
```

```python
import jax
import jax.numpy as jnp
from jax import lax
from jax.experimental import pallas as pl
from jax.experimental.pallas import tpu as pltpu
from jax.sharding import PartitionSpec as P

MESH = pl.DeviceIdType.MESH

def mod4(v):
    return lax.rem(v + 4, 4)

def place():
    row, col = lax.axis_index("row"), lax.axis_index("col")
    return [col // 4, lax.rem(col, 4), row // 2], lax.rem(row, 2)

def device(xyz, core):
    return (xyz[2] * 2 + core, xyz[0] * 4 + xyz[1])

def moved(xyz, dim, by):
    out = list(xyz)
    out[dim] = mod4(out[dim] + by)
    return out

def greet(xyz, core):
    barrier = pltpu.get_barrier_semaphore()
    for dim in range(3):
        for by in (1, -1):
            pl.semaphore_signal(barrier, inc=1, device_id=device(moved(xyz, dim, by), core), device_id_type=MESH)
    pl.semaphore_signal(barrier, inc=1, device_id=device(xyz, 1 - core), device_id_type=MESH)
    pl.semaphore_wait(barrier, 7)

ORDERS = ((0, 1, 2), (1, 2, 0), (2, 0, 1))

def gather_body(own_ref, out_ref, recv, send, near, sib_send, local):
    xyz, core = place()
    greet(xyz, core)
    half = own_ref.shape[1] // 2
    pend = []

    def push(src, dst, to, to_core, rsem, ssem):
        c = pltpu.make_async_remote_copy(src_ref=src, dst_ref=dst, send_sem=ssem, recv_sem=rsem,
                                         device_id=device(to, to_core), device_id_type=MESH)
        c.start()
        pend.append(c)

    def arrive(dst, rsem):
        pltpu.make_async_remote_copy(src_ref=dst, dst_ref=dst, send_sem=rsem, recv_sem=rsem,
                                     device_id=device(xyz, 1 - core), device_id_type=MESH).wait_recv()

    class Part:
        pass
    parts = []
    for p, (a, b, c) in enumerate(ORDERS):
        s = Part()
        s.p, s.a, s.b, s.c = p, a, b, c
        s.ia, s.ib, s.ic = xyz[a], xyz[b], xyz[c]
        s.nsend = 0
        parts.append(s)

    def block(s, ja, jb, jc, sub=None):
        r = out_ref.at[s.p, jc, jb, ja, core]
        return r if sub is None else r.at[sub]

    def group(s, jb, jc, k=None):
        return out_ref.at[s.p, jc, jb, :, core if k is None else k]

    def nsem(s):
        s.nsend += 1
        return send.at[s.p, s.nsend - 1]

    lo, hi = pl.ds(0, half), pl.ds(half, half)
    rel = lambda i, r: mod4(i + r)
    copies = []
    for s in parts:
        own = own_ref.at[s.p]
        cp = pltpu.make_async_copy(own, block(s, s.ia, s.ib, s.ic), local.at[s.p])
        cp.start()
        copies.append(cp)
        for d, by in ((0, 1), (1, -1)):
            push(own, block(s, s.ia, s.ib, s.ic), moved(xyz, s.a, by), core, recv.at[s.p, d], nsem(s))
    for s in parts:
        own = own_ref.at[s.p]
        for d, by in ((0, 1), (1, -1)):
            push(own, block(s, s.ia, s.ib, s.ic), moved(xyz, s.b, by), core, recv.at[s.p, 4 + 4 * d + 0], nsem(s))

    def send_b(s, r):
        ja = rel(s.ia, r)
        for d, by in ((0, 1), (1, -1)):
            push(block(s, ja, s.ib, s.ic), block(s, ja, s.ib, s.ic), moved(xyz, s.b, by), core,
                 recv.at[s.p, 4 + 4 * d + r], nsem(s))

    for s in parts:
        ja = rel(s.ia, -1)
        arrive(block(s, ja, s.ib, s.ic), recv.at[s.p, 0])
        push(block(s, ja, s.ib, s.ic, lo), block(s, ja, s.ib, s.ic, lo), moved(xyz, s.a, 1), core, recv.at[s.p, 2], nsem(s))
        ja2 = rel(s.ia, 1)
        arrive(block(s, ja2, s.ib, s.ic), recv.at[s.p, 1])
        push(block(s, ja2, s.ib, s.ic, hi), block(s, ja2, s.ib, s.ic, hi), moved(xyz, s.a, -1), core, recv.at[s.p, 3], nsem(s))
        send_b(s, 3)
        send_b(s, 1)

    def sib(s, jb, jc, slot):
        push(group(s, jb, jc), group(s, jb, jc), xyz, 1 - core, near.at[s.p, slot], sib_send.at[s.p, slot])

    def send_c(s, r):
        jb = rel(s.ib, r)
        for d, by in ((0, 1), (1, -1)):
            push(group(s, jb, s.ic), group(s, jb, s.ic), moved(xyz, s.c, by), core,
                 recv.at[s.p, 16 + 4 * d + r], nsem(s))
        sib(s, jb, s.ic, r)

    for s, cp in zip(parts, copies):
        ja = rel(s.ia, 2)
        arrive(block(s, ja, s.ib, s.ic, lo), recv.at[s.p, 2])
        arrive(block(s, ja, s.ib, s.ic, hi), recv.at[s.p, 3])
        send_b(s, 2)
        cp.wait()
        send_c(s, 0)
    for s in parts:
        for r in (0, 3, 1, 2):
            ja = rel(s.ia, r)
            for d, by in ((0, 1), (1, -1)):
                jb = rel(s.ib, -by)
                arrive(block(s, ja, jb, s.ic), recv.at[s.p, 4 + 4 * d + r])
                if (d == 0) == (r in (0, 3)):
                    push(block(s, ja, jb, s.ic), block(s, ja, jb, s.ic), moved(xyz, s.b, by), core,
                         recv.at[s.p, 12 + r], nsem(s))
        send_c(s, 3)
        send_c(s, 1)
    for s in parts:
        jb = rel(s.ib, 2)
        for r in (0, 3, 1, 2):
            arrive(block(s, rel(s.ia, r), jb, s.ic), recv.at[s.p, 12 + r])
        send_c(s, 2)
    for r in (0, 3, 1, 2):
        for s in parts:
            jb = rel(s.ib, r)
            for d, by in ((0, 1), (1, -1)):
                jc = rel(s.ic, -by)
                arrive(group(s, jb, jc), recv.at[s.p, 16 + 4 * d + r])
                if (d == 0) == (r in (0, 3)):
                    push(group(s, jb, jc), group(s, jb, jc), moved(xyz, s.c, by), core, recv.at[s.p, 24 + r], nsem(s))
                sib(s, jb, jc, 4 + 4 * d + r)
    for r in (0, 3, 1, 2):
        for s in parts:
            jb, jc = rel(s.ib, r), rel(s.ic, 2)
            arrive(group(s, jb, jc), recv.at[s.p, 24 + r])
            sib(s, jb, jc, 12 + r)
    for s in parts:
        for r in range(4):
            for slot, jc in ((r, s.ic), (4 + r, rel(s.ic, -1)), (8 + r, rel(s.ic, 1)), (12 + r, rel(s.ic, 2))):
                arrive(group(s, rel(s.ib, r), jc, 1 - core), near.at[s.p, slot])
    for c in pend:
        c.wait_send()

def all_gather(own):
    parts, clusters, rows, lanes = own.shape
    return pl.pallas_call(
        gather_body,
        out_shape=jax.ShapeDtypeStruct((parts, 4, 4, 4, 2, clusters, rows, lanes), jnp.float32),
        in_specs=[pl.BlockSpec(memory_space=pltpu.VMEM)],
        out_specs=pl.BlockSpec(memory_space=pl.ANY),
        scratch_shapes=[
            pltpu.SemaphoreType.DMA((3, 28)),
            pltpu.SemaphoreType.DMA((3, 28)),
            pltpu.SemaphoreType.DMA((3, 16)),
            pltpu.SemaphoreType.DMA((3, 16)),
            pltpu.SemaphoreType.DMA((3,)),
        ],
        compiler_params=pltpu.CompilerParams(collective_id=0, has_side_effects=True),
        name="torus_gather",
    )(own)


FIRST = (2, 3, 1, 0)
UP, DOWN = (2, 1), (3, 0)

def scatter_body(part_ref, out_ref, held, other, in_c, in_b, far_a, in_a,
                 load, near, near_send, rc, sc, rb, sb, ra, sa):
    xyz, core = place()
    pend = []
    rel = lambda i, r: mod4(i + r)
    info = []
    for p, (a, b, c) in enumerate(ORDERS):
        info.append((p, a, b, c, xyz[a], xyz[b], xyz[c]))

    def push(src, dst, to, to_core, rsem, ssem):
        cp = pltpu.make_async_remote_copy(src_ref=src, dst_ref=dst, send_sem=ssem, recv_sem=rsem,
                                          device_id=device(to, to_core), device_id_type=MESH)
        cp.start()
        pend.append(cp)

    def arrive(dst, rsem):
        pltpu.make_async_remote_copy(src_ref=dst, dst_ref=dst, send_sem=rsem, recv_sem=rsem,
                                     device_id=device(xyz, 1 - core), device_id_type=MESH).wait_recv()

    loads = {}
    def fetch(r4):
        for r in FIRST:
            for p, a, b, c, ia, ib, ic in info:
                jc, jb = rel(ic, r4), rel(ib, r)
                cp = pltpu.make_async_copy(part_ref.at[p, jc, jb, :, core], held.at[p, jc, jb], load.at[p, r4 * 4 + r])
                cp.start()
                loads[p, r4, r] = cp
    def swap(r4):
        for r in FIRST:
            for p, a, b, c, ia, ib, ic in info:
                jc, jb = rel(ic, r4), rel(ib, r)
                push(part_ref.at[p, jc, jb, :, 1 - core], other.at[p, jc, jb], xyz, 1 - core,
                     near.at[p, r4 * 4 + r], near_send.at[p, r4 * 4 + r])
    fetch(2)
    greet(xyz, core)
    for r4 in (2, 1, 3, 0):
        swap(r4)
        if r4 != 2:
            fetch(r4)

    def ready(p, r4, r, jc, jb):
        loads[p, r4, r].wait()
        arrive(other.at[p, jc, jb], near.at[p, r4 * 4 + r])

    for r in FIRST:
        for p, a, b, c, ia, ib, ic in info:
            jc, jb = rel(ic, 2), rel(ib, r)
            ready(p, 2, r, jc, jb)
            held[p, jc, jb] = held[p, jc, jb] + other[p, jc, jb]
            push(held.at[p, jc, jb], in_c.at[p, r], moved(xyz, c, 1 if r in UP else -1), core, rc.at[p, r], sc.at[p, r])
    for up, r, far in ((True, 3, False), (False, 2, False), (True, 0, False), (False, 1, False),
                       (True, 2, True), (False, 3, True), (True, 1, True), (False, 0, True)):
        for p, a, b, c, ia, ib, ic in info:
            by = 1 if up else -1
            jc, jb = rel(ic, by), rel(ib, r)
            ready(p, 1 if up else 3, r, jc, jb)
            if far:
                arrive(in_c.at[p, r], rc.at[p, r])
                held[p, jc, jb] = held[p, jc, jb] + other[p, jc, jb] + in_c[p, r]
            else:
                held[p, jc, jb] = held[p, jc, jb] + other[p, jc, jb]
            slot = (4 if up else 8) + r
            push(held.at[p, jc, jb], in_c.at[p, slot], moved(xyz, c, by), core, rc.at[p, slot], sc.at[p, slot])
    def finish_c(r):
        for p, a, b, c, ia, ib, ic in info:
            jc, jb = ic, rel(ib, r)
            ready(p, 0, r, jc, jb)
            arrive(in_c.at[p, 4 + r], rc.at[p, 4 + r])
            arrive(in_c.at[p, 8 + r], rc.at[p, 8 + r])
            held[p, jc, jb] = held[p, jc, jb] + other[p, jc, jb] + (in_c[p, 4 + r] + in_c[p, 8 + r])
    def send_b(p, b, jc, jb, ja, slot, by):
        push(held.at[p, jc, jb, ja], in_b.at[p, slot], moved(xyz, b, by), core, rb.at[p, slot], sb.at[p, slot])
    finish_c(2)
    for q in FIRST:
        for p, a, b, c, ia, ib, ic in info:
            send_b(p, b, ic, rel(ib, 2), rel(ia, q), q, 1 if q in UP else -1)
    finish_c(3)
    finish_c(1)
    for q in (3, 0):
        for p, a, b, c, ia, ib, ic in info:
            send_b(p, b, ic, rel(ib, 1), rel(ia, q), 4 + q, 1)
    for q in (2, 1):
        for p, a, b, c, ia, ib, ic in info:
            send_b(p, b, ic, rel(ib, 3), rel(ia, q), 8 + q, -1)
    for up, q in ((True, 2), (False, 3), (True, 1), (False, 0)):
        for p, a, b, c, ia, ib, ic in info:
            by = 1 if up else -1
            jc, jb, ja = ic, rel(ib, by), rel(ia, q)
            arrive(in_b.at[p, q], rb.at[p, q])
            held[p, jc, jb, ja] = held[p, jc, jb, ja] + in_b[p, q]
            send_b(p, b, jc, jb, ja, (4 if up else 8) + q, by)
    finish_c(0)
    def finish_b(q):
        for p, a, b, c, ia, ib, ic in info:
            ja = rel(ia, q)
            arrive(in_b.at[p, 4 + q], rb.at[p, 4 + q])
            arrive(in_b.at[p, 8 + q], rb.at[p, 8 + q])
            held[p, ic, ib, ja] = held[p, ic, ib, ja] + (in_b[p, 4 + q] + in_b[p, 8 + q])
    finish_b(2)
    lo, hi = pl.ds(0, 8), pl.ds(8, 8)
    for p, a, b, c, ia, ib, ic in info:
        blk = held.at[p, ic, ib, rel(ia, 2)]
        push(blk.at[lo], far_a.at[p, 0], moved(xyz, a, 1), core, ra.at[p, 0], sa.at[p, 0])
        push(blk.at[hi], far_a.at[p, 1], moved(xyz, a, -1), core, ra.at[p, 1], sa.at[p, 1])
    finish_b(1)
    finish_b(3)
    for p, a, b, c, ia, ib, ic in info:
        ja = rel(ia, 1)
        arrive(far_a.at[p, 0], ra.at[p, 0])
        held[p, ic, ib, ja, 0:8] = held[p, ic, ib, ja, 0:8] + far_a[p, 0]
        push(held.at[p, ic, ib, ja], in_a.at[p, 0], moved(xyz, a, 1), core, ra.at[p, 2], sa.at[p, 2])
        ja = rel(ia, 3)
        arrive(far_a.at[p, 1], ra.at[p, 1])
        held[p, ic, ib, ja, 8:16] = held[p, ic, ib, ja, 8:16] + far_a[p, 1]
        push(held.at[p, ic, ib, ja], in_a.at[p, 1], moved(xyz, a, -1), core, ra.at[p, 3], sa.at[p, 3])
    finish_b(0)
    for p, a, b, c, ia, ib, ic in info:
        arrive(in_a.at[p, 0], ra.at[p, 2])
        arrive(in_a.at[p, 1], ra.at[p, 3])
        out_ref[p] = held[p, ic, ib, ia] + (in_a[p, 0] + in_a[p, 1])
    for cp in pend:
        cp.wait_send()

def reduce_scatter(part):
    clusters, nodes = part.shape[-2:]
    D = pltpu.SemaphoreType.DMA
    V = lambda *s: pltpu.VMEM(s + (clusters, nodes), jnp.float32)
    return pl.pallas_call(
        scatter_body,
        out_shape=jax.ShapeDtypeStruct((3, clusters, nodes), jnp.float32),
        in_specs=[pl.BlockSpec(memory_space=pl.ANY)],
        out_specs=pl.BlockSpec(memory_space=pltpu.VMEM),
        scratch_shapes=[V(3, 4, 4, 4), V(3, 4, 4, 4), V(3, 12, 4), V(3, 12),
                        pltpu.VMEM((3, 2, clusters // 2, nodes), jnp.float32), V(3, 2),
                        D((3, 16)), D((3, 16)), D((3, 16)), D((3, 12)), D((3, 12)), D((3, 12)), D((3, 12)),
                        D((3, 4)), D((3, 4))],
        compiler_params=pltpu.CompilerParams(collective_id=1, has_side_effects=True, vmem_limit_bytes=40 * 2**20),
        name="torus_scatter",
    )(part)

ROWS = 32
UNROLL = 2

def pieces(value):
    high = value.astype(jnp.bfloat16)
    rest = value - high.astype(jnp.float32)
    mid = rest.astype(jnp.bfloat16)
    low = (rest - mid.astype(jnp.float32)).astype(jnp.bfloat16)
    return high, mid, low


def coeff_body(disp_ref, coords_ref, inverse_ref, table_ref):
    c = pl.program_id(0)
    nodes = inverse_ref.shape[-1]
    left = jnp.concatenate([disp_ref[i, pl.ds(c, 1), :] for i in range(3)] + [jnp.zeros((5, nodes), jnp.float32)], axis=0)
    lh = left.astype(jnp.bfloat16)
    ll = (left - lh.astype(jnp.float32)).astype(jnp.bfloat16)
    both = jnp.concatenate([lh, ll], axis=0)
    whole = inverse_ref[0]
    ih = whole.astype(jnp.bfloat16)
    il = (whole - ih.astype(jnp.float32)).astype(jnp.bfloat16)
    top = jnp.dot(both, ih, preferred_element_type=jnp.float32)
    low = jnp.dot(both, il, preferred_element_type=jnp.float32)
    res = top[0:8] + (top[8:16] + low[0:8])
    for i in range(6):
        row = coords_ref[i, pl.ds(c, 1), :] if i < 3 else res[i - 3:i - 2]
        for q in range(4):
            table_ref[i // 2, c, pl.ds((i % 2) * 4 + q, 1), :] = row[:, q * 128:(q + 1) * 128]


def own_table(node_disp, node_coords, inverse):
    clusters, nodes = inverse.shape[0], inverse.shape[1]
    whole = pl.BlockSpec((3, clusters, nodes), lambda c: (0, 0, 0))
    return pl.pallas_call(
        coeff_body,
        grid=(clusters,),
        out_shape=jax.ShapeDtypeStruct((3, clusters, 8, 128), jnp.float32),
        in_specs=[whole, whole, pl.BlockSpec((1, nodes, nodes), lambda c: (c, 0, 0))],
        out_specs=pl.BlockSpec((3, clusters, 8, 128), lambda c: (0, 0, 0, 0)),
        name="coefficients",
    )(node_disp, node_coords, inverse)


def pairs_body(ids_ref, pts_ref, frc_ref, lev_ref, table_ref, disp_ref, part_ref,
               rows, spots, raw, packed, mark, tally, flat, jobs, count, sem, sem2):
    tiles, slots = ids_ref.shape
    points = pts_ref.shape[-1]
    total = tiles * slots

    def start(q, carry):
        cid = ids_ref[q // slots, q % slots]
        l, dev = cid & 15, cid >> 4
        core, z = (dev >> 4) & 1, dev >> 5
        y, x = dev & 3, (dev >> 2) & 3
        for p, (a, b, c) in enumerate(((x, y, z), (y, z, x), (z, x, y))):
            f = (((c * 4 + b) * 4 + a) * 2 + core) * 16 + l
            flat[p, q] = f
            pltpu.make_async_copy(table_ref.at[p, pl.ds(pl.multiple_of(f * 8, 8), 8), :],
                                  rows.at[p, pl.ds(pl.multiple_of(q * 8, 8), 8), :], sem.at[p]).start()
        return carry
    lax.fori_loop(0, total, start, 0)

    def clear(g, carry):
        part_ref[0, pl.ds(pl.multiple_of(g * 16, 16), 16), :] = jnp.zeros((16, part_ref.shape[2]), jnp.float32)
        part_ref[1, pl.ds(pl.multiple_of(g * 16, 16), 16), :] = jnp.zeros((16, part_ref.shape[2]), jnp.float32)
        part_ref[2, pl.ds(pl.multiple_of(g * 16, 16), 16), :] = jnp.zeros((16, part_ref.shape[2]), jnp.float32)
        return carry
    lax.fori_loop(0, part_ref.shape[1] // 16, clear, 0)
    disp_ref[...] = jnp.zeros(disp_ref.shape, jnp.float32)

    def columns(t, carry):
        level = lev_ref[t].astype(jnp.float32) + 1.0
        weight = level / jnp.sum(level, axis=0, keepdims=True)
        raw[t, 6:14, :] = weight
        raw[t, 14:16, :] = jnp.zeros((2, points), jnp.float32)
        for i in range(3):
            raw[t, i:i + 1, :] = pts_ref[i, pl.ds(t, 1), :]
            raw[t, 3 + i:4 + i, :] = frc_ref[i, pl.ds(t, 1), :]
        h, m, l = pieces(raw[t])
        packed[t, 0:16, :] = h
        packed[t, 16:32, :] = m
        packed[t, 32:48, :] = l
        return carry
    lax.fori_loop(0, tiles, columns, 0, unroll=2)

    for p in range(3):
        pltpu.make_async_copy(table_ref.at[p, pl.ds(0, total * 8), :], rows.at[p], sem.at[p]).wait()

    def near(t, carry):
        dist = None
        for i in range(3):
            base = t * slots * 8 + (4 if i == 1 else 0)
            chunk = [rows[i // 2, pl.ds(base + r, slots, stride=8), :] for r in range(4)]
            low = jnp.minimum(jnp.minimum(chunk[0], chunk[1]), jnp.minimum(chunk[2], chunk[3]))
            high = jnp.maximum(jnp.maximum(chunk[0], chunk[1]), jnp.maximum(chunk[2], chunk[3]))
            low = jnp.min(low, axis=1, keepdims=True)
            high = jnp.max(high, axis=1, keepdims=True)
            at = pts_ref[i, pl.ds(t, 1), :]
            gap = jnp.maximum(jnp.maximum(low - at, at - high), 0.0)
            dist = gap * gap if dist is None else dist + gap * gap
        mark[pl.ds(pl.multiple_of(t * slots, slots), slots), :] = jnp.where(dist < 1.0001, 1.0, 0.0)
        return carry
    lax.fori_loop(0, tiles, near, 0, unroll=2)

    before = (lax.broadcasted_iota(jnp.int32, (points, points), 0) < lax.broadcasted_iota(jnp.int32, (points, points), 1))
    before = jnp.where(before, 1.0, 0.0).astype(jnp.bfloat16)
    flags = mark[...]
    ones = jnp.ones((16, points), jnp.bfloat16)
    fb = flags.astype(jnp.bfloat16)
    rank = jnp.dot(fb, before, preferred_element_type=jnp.float32)
    spots[...] = jnp.where(flags > 0.5, rank, -1.0)
    sums = lax.dot_general(ones, fb, (((1,), (1,)), ((), ())), preferred_element_type=jnp.float32)
    tally[...] = sums[0:8].astype(jnp.int32)
    cp = pltpu.make_async_copy(tally, count, sem2)
    cp.start()
    cp.wait()

    def list_pair(q, m):
        n = (count[0, q] + (ROWS - 1)) // ROWS
        def put(j, m):
            jobs[m] = q * 16 + j
            return m + 1
        return lax.fori_loop(0, n, put, m)
    made = lax.fori_loop(0, total, list_pair, 0)
    for u in range(UNROLL - 1):
        jobs[made + u] = points // ROWS
    trips = (made + UNROLL - 1) // UNROLL

    place32 = lax.broadcasted_iota(jnp.int32, (ROWS, points), 0).astype(jnp.float32)
    lane16 = lax.broadcasted_iota(jnp.int32, (ROWS, 16), 1)
    lane = lax.broadcasted_iota(jnp.int32, (ROWS, 128), 1)

    def one(job):
        q, j = job >> 4, job & 15
        t, k = q // slots, q % slots
        pick = jnp.where(place32 + (j * ROWS).astype(jnp.float32) == spots[pl.ds(q, 1), :], 1.0, 0.0).astype(jnp.bfloat16)
        got = lax.dot_general(pick, packed[t], (((1,), (1,)), ((), ())), preferred_element_type=jnp.float32)
        got = got[:, 0:16] + (got[:, 16:32] + got[:, 32:48])
        px, py, pz, fx, fy, fz = [got[:, i:i + 1] for i in range(6)]
        weight = jnp.sum(jnp.where(lane16 == 6 + k, got, 0.0), axis=1, keepdims=True)
        shown = [None] * 3
        loads = [[], [], []]
        for g in range(4):
            base = q * 8 + g
            dx = px - rows[0, pl.ds(base, 1), :]
            dy = py - rows[0, pl.ds(base + 4, 1), :]
            dz = pz - rows[1, pl.ds(base, 1), :]
            d2 = jnp.maximum(dx * dx + dy * dy + dz * dz, 1e-30)
            u = jnp.maximum(1.0 - d2 * lax.rsqrt(d2), 0.0)
            u2 = u * u
            val = (u2 * u2) * (5.0 - 4.0 * u) * weight
            for i, (pp, off) in enumerate(((1, 4), (2, 0), (2, 4))):
                term = val * rows[pp, pl.ds(base + off, 1), :]
                shown[i] = term if shown[i] is None else shown[i] + term
            for i, f in enumerate((fx, fy, fz)):
                loads[i].append(jnp.sum(val * f, axis=0, keepdims=True))
        cols = [jnp.sum(s, axis=1, keepdims=True) for s in shown]
        d = jnp.where(lane == 0, cols[0], jnp.where(lane == 1, cols[1], jnp.where(lane == 2, cols[2], 0.0)))
        dt = jnp.transpose(d)[0:8]
        dh = dt.astype(jnp.bfloat16)
        dl = (dt - dh.astype(jnp.float32)).astype(jnp.bfloat16)
        back = jnp.dot(jnp.concatenate([dh, dl], axis=0), pick, preferred_element_type=jnp.float32)
        back = back[0:8] + back[8:16]
        return q, t, back, [jnp.concatenate(l, axis=1) for l in loads]

    def trip(n, carry):
        done = [one(jobs[n * UNROLL + u]) for u in range(UNROLL)]
        for q, t, back, loads in done:
            for i in range(3):
                disp_ref[i, pl.ds(t, 1), :] += back[i:i + 1]
                part_ref[i, pl.ds(flat[i, q], 1), :] += loads[i]
        return carry
    lax.fori_loop(0, trips, trip, 0)


def pairs(ids, pts, frc, lev, table):
    tiles, slots = ids.shape
    points = pts.shape[-1]
    total = tiles * slots
    clusters = table.shape[1] // 8
    vm = pl.BlockSpec(memory_space=pltpu.VMEM)
    V = lambda s, d=jnp.float32: pltpu.VMEM(s, d)
    return pl.pallas_call(
        pairs_body,
        out_shape=(jax.ShapeDtypeStruct(pts.shape, jnp.float32), jax.ShapeDtypeStruct((3, clusters, 512), jnp.float32)),
        in_specs=[pl.BlockSpec(memory_space=pltpu.SMEM), vm, vm, vm, pl.BlockSpec(memory_space=pl.ANY)],
        out_specs=(vm, vm),
        scratch_shapes=[
            V((3, total * 8, 128)), V((total, points)), V((tiles, 16, points)), V((tiles, 48, points), jnp.bfloat16),
            V((total, points)), V((8, total), jnp.int32),
            pltpu.SMEM((3, total), jnp.int32), pltpu.SMEM((total * 8 + 8,), jnp.int32), pltpu.SMEM((8, total), jnp.int32),
            pltpu.SemaphoreType.DMA((3,)), pltpu.SemaphoreType.DMA,
        ],
        compiler_params=pltpu.CompilerParams(vmem_limit_bytes=40 * 2**20),
        name="pairs",
    )(ids, pts, frc, lev, table)


def on_device(point_coords, fluid_force, tile_clusters, pu_level, node_coords, node_disp, inverse):
    turn = lambda v: jnp.transpose(v, (1, 0, 2))
    table = all_gather(own_table(turn(node_disp), turn(node_coords), inverse))
    table = table.reshape(3, -1, 128)
    shown, part = pairs(tile_clusters, turn(point_coords), turn(fluid_force), pu_level, table)
    force = reduce_scatter(part.reshape(3, 4, 4, 4, 2, node_coords.shape[0], node_coords.shape[2]))
    return turn(shown), turn(force)


def solution(mesh):
    spec = P(("row", "col"), None, None)
    return jax.shard_map(
        on_device,
        mesh=mesh,
        in_specs=(spec, spec, P(("row", "col"), None), spec, spec, spec, spec),
        out_specs=(spec, spec),
        check_vma=False,
    )
```

```python
import jax
import jax.numpy as jnp
from jax import lax
from jax.experimental import pallas as pl
from jax.experimental.pallas import tpu as pltpu
from jax.sharding import PartitionSpec as P

MESH = pl.DeviceIdType.MESH

def mod4(v):
    return lax.rem(v + 4, 4)

def place():
    row, col = lax.axis_index("row"), lax.axis_index("col")
    return [col // 4, lax.rem(col, 4), row // 2], lax.rem(row, 2)

def device(xyz, core):
    return (xyz[2] * 2 + core, xyz[0] * 4 + xyz[1])

def moved(xyz, dim, by):
    out = list(xyz)
    out[dim] = mod4(out[dim] + by)
    return out

def greet(xyz, core):
    barrier = pltpu.get_barrier_semaphore()
    for dim in range(3):
        for by in (1, -1):
            pl.semaphore_signal(barrier, inc=1, device_id=device(moved(xyz, dim, by), core), device_id_type=MESH)
    pl.semaphore_signal(barrier, inc=1, device_id=device(xyz, 1 - core), device_id_type=MESH)
    pl.semaphore_wait(barrier, 7)

ORDERS = ((0, 1, 2), (1, 2, 0), (2, 0, 1))

def gather_body(own_ref, out_ref, recv, send, near, sib_send, local):
    xyz, core = place()
    greet(xyz, core)
    half = own_ref.shape[1] // 2
    pend = []

    def push(src, dst, to, to_core, rsem, ssem):
        c = pltpu.make_async_remote_copy(src_ref=src, dst_ref=dst, send_sem=ssem, recv_sem=rsem,
                                         device_id=device(to, to_core), device_id_type=MESH)
        c.start()
        pend.append(c)

    def arrive(dst, rsem):
        pltpu.make_async_remote_copy(src_ref=dst, dst_ref=dst, send_sem=rsem, recv_sem=rsem,
                                     device_id=device(xyz, 1 - core), device_id_type=MESH).wait_recv()

    class Part:
        pass
    parts = []
    for p, (a, b, c) in enumerate(ORDERS):
        s = Part()
        s.p, s.a, s.b, s.c = p, a, b, c
        s.ia, s.ib, s.ic = xyz[a], xyz[b], xyz[c]
        s.nsend = 0
        parts.append(s)

    def block(s, ja, jb, jc, sub=None):
        r = out_ref.at[s.p, jc, jb, ja, core]
        return r if sub is None else r.at[sub]

    def group(s, jb, jc, k=None):
        return out_ref.at[s.p, jc, jb, :, core if k is None else k]

    def nsem(s):
        s.nsend += 1
        return send.at[s.p, s.nsend - 1]

    lo, hi = pl.ds(0, half), pl.ds(half, half)
    rel = lambda i, r: mod4(i + r)
    copies = []
    for s in parts:
        own = own_ref.at[s.p]
        cp = pltpu.make_async_copy(own, block(s, s.ia, s.ib, s.ic), local.at[s.p])
        cp.start()
        copies.append(cp)
        for d, by in ((0, 1), (1, -1)):
            push(own, block(s, s.ia, s.ib, s.ic), moved(xyz, s.a, by), core, recv.at[s.p, d], nsem(s))
    for s in parts:
        own = own_ref.at[s.p]
        for d, by in ((0, 1), (1, -1)):
            push(own, block(s, s.ia, s.ib, s.ic), moved(xyz, s.b, by), core, recv.at[s.p, 4 + 4 * d + 0], nsem(s))

    def send_b(s, r):
        ja = rel(s.ia, r)
        for d, by in ((0, 1), (1, -1)):
            push(block(s, ja, s.ib, s.ic), block(s, ja, s.ib, s.ic), moved(xyz, s.b, by), core,
                 recv.at[s.p, 4 + 4 * d + r], nsem(s))

    for s in parts:
        ja = rel(s.ia, -1)
        arrive(block(s, ja, s.ib, s.ic), recv.at[s.p, 0])
        push(block(s, ja, s.ib, s.ic, lo), block(s, ja, s.ib, s.ic, lo), moved(xyz, s.a, 1), core, recv.at[s.p, 2], nsem(s))
        ja2 = rel(s.ia, 1)
        arrive(block(s, ja2, s.ib, s.ic), recv.at[s.p, 1])
        push(block(s, ja2, s.ib, s.ic, hi), block(s, ja2, s.ib, s.ic, hi), moved(xyz, s.a, -1), core, recv.at[s.p, 3], nsem(s))
        send_b(s, 3)
        send_b(s, 1)

    def sib(s, jb, jc, slot):
        push(group(s, jb, jc), group(s, jb, jc), xyz, 1 - core, near.at[s.p, slot], sib_send.at[s.p, slot])

    def send_c(s, r):
        jb = rel(s.ib, r)
        for d, by in ((0, 1), (1, -1)):
            push(group(s, jb, s.ic), group(s, jb, s.ic), moved(xyz, s.c, by), core,
                 recv.at[s.p, 16 + 4 * d + r], nsem(s))
        sib(s, jb, s.ic, r)

    for s, cp in zip(parts, copies):
        ja = rel(s.ia, 2)
        arrive(block(s, ja, s.ib, s.ic, lo), recv.at[s.p, 2])
        arrive(block(s, ja, s.ib, s.ic, hi), recv.at[s.p, 3])
        send_b(s, 2)
        cp.wait()
        send_c(s, 0)
    for s in parts:
        for r in (0, 3, 1, 2):
            ja = rel(s.ia, r)
            for d, by in ((0, 1), (1, -1)):
                jb = rel(s.ib, -by)
                arrive(block(s, ja, jb, s.ic), recv.at[s.p, 4 + 4 * d + r])
                if (d == 0) == (r in (0, 3)):
                    push(block(s, ja, jb, s.ic), block(s, ja, jb, s.ic), moved(xyz, s.b, by), core,
                         recv.at[s.p, 12 + r], nsem(s))
        send_c(s, 3)
        send_c(s, 1)
    for s in parts:
        jb = rel(s.ib, 2)
        for r in (0, 3, 1, 2):
            arrive(block(s, rel(s.ia, r), jb, s.ic), recv.at[s.p, 12 + r])
        send_c(s, 2)
    for r in (0, 3, 1, 2):
        for s in parts:
            jb = rel(s.ib, r)
            for d, by in ((0, 1), (1, -1)):
                jc = rel(s.ic, -by)
                arrive(group(s, jb, jc), recv.at[s.p, 16 + 4 * d + r])
                if (d == 0) == (r in (0, 3)):
                    push(group(s, jb, jc), group(s, jb, jc), moved(xyz, s.c, by), core, recv.at[s.p, 24 + r], nsem(s))
                sib(s, jb, jc, 4 + 4 * d + r)
    for r in (0, 3, 1, 2):
        for s in parts:
            jb, jc = rel(s.ib, r), rel(s.ic, 2)
            arrive(group(s, jb, jc), recv.at[s.p, 24 + r])
            sib(s, jb, jc, 12 + r)
    for s in parts:
        for r in range(4):
            for slot, jc in ((r, s.ic), (4 + r, rel(s.ic, -1)), (8 + r, rel(s.ic, 1)), (12 + r, rel(s.ic, 2))):
                arrive(group(s, rel(s.ib, r), jc, 1 - core), near.at[s.p, slot])
    for c in pend:
        c.wait_send()

def all_gather(own):
    parts, clusters, rows, lanes = own.shape
    return pl.pallas_call(
        gather_body,
        out_shape=jax.ShapeDtypeStruct((parts, 4, 4, 4, 2, clusters, rows, lanes), jnp.float32),
        in_specs=[pl.BlockSpec(memory_space=pltpu.VMEM)],
        out_specs=pl.BlockSpec(memory_space=pltpu.VMEM),
        scratch_shapes=[
            pltpu.SemaphoreType.DMA((3, 28)),
            pltpu.SemaphoreType.DMA((3, 28)),
            pltpu.SemaphoreType.DMA((3, 16)),
            pltpu.SemaphoreType.DMA((3, 16)),
            pltpu.SemaphoreType.DMA((3,)),
        ],
        compiler_params=pltpu.CompilerParams(collective_id=0, has_side_effects=True, vmem_limit_bytes=2 * 2**20),
        name="torus_gather",
    )(own)


FIRST = (2, 3, 1, 0)
UP, DOWN = (2, 1), (3, 0)

def scatter_body(part_ref, out_ref, held, other, in_c, in_b, far_a, in_a,
                 near, near_send, rc, sc, rb, sb, ra, sa):
    xyz, core = place()
    pend = []
    rel = lambda i, r: mod4(i + r)
    info = []
    for p, (a, b, c) in enumerate(ORDERS):
        info.append((p, a, b, c, xyz[a], xyz[b], xyz[c]))

    def push(src, dst, to, to_core, rsem, ssem):
        cp = pltpu.make_async_remote_copy(src_ref=src, dst_ref=dst, send_sem=ssem, recv_sem=rsem,
                                          device_id=device(to, to_core), device_id_type=MESH)
        cp.start()
        pend.append(cp)

    def arrive(dst, rsem):
        pltpu.make_async_remote_copy(src_ref=dst, dst_ref=dst, send_sem=rsem, recv_sem=rsem,
                                     device_id=device(xyz, 1 - core), device_id_type=MESH).wait_recv()

    def swap(r4):
        for r in FIRST:
            for p, a, b, c, ia, ib, ic in info:
                jc, jb = rel(ic, r4), rel(ib, r)
                push(part_ref.at[p, jc, jb, :, 1 - core], other.at[p, jc, jb], xyz, 1 - core,
                     near.at[p, r4 * 4 + r], near_send.at[p, r4 * 4 + r])
    greet(xyz, core)
    for r4 in (2, 1, 3, 0):
        swap(r4)

    def ready(p, r4, r, jc, jb):
        arrive(other.at[p, jc, jb], near.at[p, r4 * 4 + r])

    for r in FIRST:
        for p, a, b, c, ia, ib, ic in info:
            jc, jb = rel(ic, 2), rel(ib, r)
            ready(p, 2, r, jc, jb)
            held[p, jc, jb] = part_ref[p, jc, jb, :, core] + other[p, jc, jb]
            push(held.at[p, jc, jb], in_c.at[p, r], moved(xyz, c, 1 if r in UP else -1), core, rc.at[p, r], sc.at[p, r])
    for up, r, far in ((True, 3, False), (False, 2, False), (True, 0, False), (False, 1, False),
                       (True, 2, True), (False, 3, True), (True, 1, True), (False, 0, True)):
        for p, a, b, c, ia, ib, ic in info:
            by = 1 if up else -1
            jc, jb = rel(ic, by), rel(ib, r)
            ready(p, 1 if up else 3, r, jc, jb)
            if far:
                arrive(in_c.at[p, r], rc.at[p, r])
                held[p, jc, jb] = part_ref[p, jc, jb, :, core] + other[p, jc, jb] + in_c[p, r]
            else:
                held[p, jc, jb] = part_ref[p, jc, jb, :, core] + other[p, jc, jb]
            slot = (4 if up else 8) + r
            push(held.at[p, jc, jb], in_c.at[p, slot], moved(xyz, c, by), core, rc.at[p, slot], sc.at[p, slot])
    def finish_c(r):
        for p, a, b, c, ia, ib, ic in info:
            jc, jb = ic, rel(ib, r)
            ready(p, 0, r, jc, jb)
            arrive(in_c.at[p, 4 + r], rc.at[p, 4 + r])
            arrive(in_c.at[p, 8 + r], rc.at[p, 8 + r])
            held[p, jc, jb] = part_ref[p, jc, jb, :, core] + other[p, jc, jb] + (in_c[p, 4 + r] + in_c[p, 8 + r])
    def send_b(p, b, jc, jb, ja, slot, by):
        push(held.at[p, jc, jb, ja], in_b.at[p, slot], moved(xyz, b, by), core, rb.at[p, slot], sb.at[p, slot])
    finish_c(2)
    for q in FIRST:
        for p, a, b, c, ia, ib, ic in info:
            send_b(p, b, ic, rel(ib, 2), rel(ia, q), q, 1 if q in UP else -1)
    finish_c(3)
    finish_c(1)
    for q in (3, 0):
        for p, a, b, c, ia, ib, ic in info:
            send_b(p, b, ic, rel(ib, 1), rel(ia, q), 4 + q, 1)
    for q in (2, 1):
        for p, a, b, c, ia, ib, ic in info:
            send_b(p, b, ic, rel(ib, 3), rel(ia, q), 8 + q, -1)
    for up, q in ((True, 2), (False, 3), (True, 1), (False, 0)):
        for p, a, b, c, ia, ib, ic in info:
            by = 1 if up else -1
            jc, jb, ja = ic, rel(ib, by), rel(ia, q)
            arrive(in_b.at[p, q], rb.at[p, q])
            held[p, jc, jb, ja] = held[p, jc, jb, ja] + in_b[p, q]
            send_b(p, b, jc, jb, ja, (4 if up else 8) + q, by)
    finish_c(0)
    def finish_b(q):
        for p, a, b, c, ia, ib, ic in info:
            ja = rel(ia, q)
            arrive(in_b.at[p, 4 + q], rb.at[p, 4 + q])
            arrive(in_b.at[p, 8 + q], rb.at[p, 8 + q])
            held[p, ic, ib, ja] = held[p, ic, ib, ja] + (in_b[p, 4 + q] + in_b[p, 8 + q])
    finish_b(2)
    lo, hi = pl.ds(0, 8), pl.ds(8, 8)
    for p, a, b, c, ia, ib, ic in info:
        blk = held.at[p, ic, ib, rel(ia, 2)]
        push(blk.at[lo], far_a.at[p, 0], moved(xyz, a, 1), core, ra.at[p, 0], sa.at[p, 0])
        push(blk.at[hi], far_a.at[p, 1], moved(xyz, a, -1), core, ra.at[p, 1], sa.at[p, 1])
    finish_b(1)
    finish_b(3)
    for p, a, b, c, ia, ib, ic in info:
        ja = rel(ia, 1)
        arrive(far_a.at[p, 0], ra.at[p, 0])
        held[p, ic, ib, ja, 0:8] = held[p, ic, ib, ja, 0:8] + far_a[p, 0]
        push(held.at[p, ic, ib, ja], in_a.at[p, 0], moved(xyz, a, 1), core, ra.at[p, 2], sa.at[p, 2])
        ja = rel(ia, 3)
        arrive(far_a.at[p, 1], ra.at[p, 1])
        held[p, ic, ib, ja, 8:16] = held[p, ic, ib, ja, 8:16] + far_a[p, 1]
        push(held.at[p, ic, ib, ja], in_a.at[p, 1], moved(xyz, a, -1), core, ra.at[p, 3], sa.at[p, 3])
    finish_b(0)
    for p, a, b, c, ia, ib, ic in info:
        arrive(in_a.at[p, 0], ra.at[p, 2])
        arrive(in_a.at[p, 1], ra.at[p, 3])
        out_ref[p] = held[p, ic, ib, ia] + (in_a[p, 0] + in_a[p, 1])
    for cp in pend:
        cp.wait_send()

def reduce_scatter(part):
    clusters, nodes = part.shape[-2:]
    D = pltpu.SemaphoreType.DMA
    V = lambda *s: pltpu.VMEM(s + (clusters, nodes), jnp.float32)
    return pl.pallas_call(
        scatter_body,
        out_shape=jax.ShapeDtypeStruct((3, clusters, nodes), jnp.float32),
        in_specs=[pl.BlockSpec(memory_space=pltpu.VMEM)],
        out_specs=pl.BlockSpec(memory_space=pltpu.VMEM),
        scratch_shapes=[V(3, 4, 4, 4), V(3, 4, 4, 4), V(3, 12, 4), V(3, 12),
                        pltpu.VMEM((3, 2, clusters // 2, nodes), jnp.float32), V(3, 2),
                        D((3, 16)), D((3, 16)), D((3, 12)), D((3, 12)), D((3, 12)), D((3, 12)),
                        D((3, 4)), D((3, 4))],
        compiler_params=pltpu.CompilerParams(collective_id=1, has_side_effects=True, vmem_limit_bytes=24 * 2**20),
        name="torus_scatter",
    )(part)

ROWS = 32
BATCH = 32
WIDE = 32
UNROLL = 2

def pieces(value):
    high = value.astype(jnp.bfloat16)
    rest = value - high.astype(jnp.float32)
    mid = rest.astype(jnp.bfloat16)
    low = (rest - mid.astype(jnp.float32)).astype(jnp.bfloat16)
    return high, mid, low


def coeff_body(disp_ref, coords_ref, inverse_ref, table_ref):
    c = pl.program_id(0)
    nodes = inverse_ref.shape[-1]
    left = jnp.concatenate([disp_ref[i, pl.ds(c, 1), :] for i in range(3)] + [jnp.zeros((5, nodes), jnp.float32)], axis=0)
    lh = left.astype(jnp.bfloat16)
    ll = (left - lh.astype(jnp.float32)).astype(jnp.bfloat16)
    both = jnp.concatenate([lh, ll], axis=0)
    whole = inverse_ref[0]
    ih = whole.astype(jnp.bfloat16)
    il = (whole - ih.astype(jnp.float32)).astype(jnp.bfloat16)
    top = jnp.dot(both, ih, preferred_element_type=jnp.float32)
    low = jnp.dot(both, il, preferred_element_type=jnp.float32)
    res = top[0:8] + (top[8:16] + low[0:8])
    for i in range(6):
        row = coords_ref[i, pl.ds(c, 1), :] if i < 3 else res[i - 3:i - 2]
        for q in range(4):
            table_ref[i // 2, c, pl.ds((i % 2) * 4 + q, 1), :] = row[:, q * 128:(q + 1) * 128]


def own_table(node_disp, node_coords, inverse):
    clusters, nodes = inverse.shape[0], inverse.shape[1]
    whole = pl.BlockSpec((3, clusters, nodes), lambda c: (0, 0, 0))
    return pl.pallas_call(
        coeff_body,
        grid=(clusters,),
        out_shape=jax.ShapeDtypeStruct((3, clusters, 8, 128), jnp.float32),
        in_specs=[whole, whole, pl.BlockSpec((1, nodes, nodes), lambda c: (c, 0, 0))],
        out_specs=pl.BlockSpec((3, clusters, 8, 128), lambda c: (0, 0, 0, 0)),
        name="coefficients",
    )(node_disp, node_coords, inverse)


def pairs_body(ids_ref, pts_ref, frc_ref, lev_ref, table_ref, disp_ref, part_ref,
               rows, spots, raw, packed, mark, picks, wide, moved_sum, spread_all, tally, flat, jobs, count, sem2):
    tiles, slots = ids_ref.shape
    points = pts_ref.shape[-1]
    total = tiles * slots

    def fetch(t, carry):
        for k in range(slots):
            cid = ids_ref[t, k]
            l, dev = cid & 15, cid >> 4
            core, z = (dev >> 4) & 1, dev >> 5
            y, x = dev & 3, (dev >> 2) & 3
            for p, (a, b, c) in enumerate(((x, y, z), (y, z, x), (z, x, y))):
                f = (((c * 4 + b) * 4 + a) * 2 + core) * 16 + l
                flat[p, t * slots + k] = f
                rows[p, pl.ds(pl.multiple_of((t * slots + k) * 8, 8), 8), :] = table_ref[p, pl.ds(pl.multiple_of(f * 8, 8), 8), :]
        return carry
    lax.fori_loop(0, tiles, fetch, 0)

    def clear(g, carry):
        part_ref[0, pl.ds(pl.multiple_of(g * 16, 16), 16), :] = jnp.zeros((16, part_ref.shape[2]), jnp.float32)
        part_ref[1, pl.ds(pl.multiple_of(g * 16, 16), 16), :] = jnp.zeros((16, part_ref.shape[2]), jnp.float32)
        part_ref[2, pl.ds(pl.multiple_of(g * 16, 16), 16), :] = jnp.zeros((16, part_ref.shape[2]), jnp.float32)
        return carry
    lax.fori_loop(0, part_ref.shape[1] // 16, clear, 0)
    disp_ref[...] = jnp.zeros(disp_ref.shape, jnp.float32)

    def columns(t, carry):
        level = lev_ref[t].astype(jnp.float32) + 1.0
        weight = level / jnp.sum(level, axis=0, keepdims=True)
        raw[t, 6:14, :] = weight * 4.0
        raw[t, 14:16, :] = jnp.zeros((2, points), jnp.float32)
        for i in range(3):
            raw[t, i:i + 1, :] = pts_ref[i, pl.ds(t, 1), :]
            raw[t, 3 + i:4 + i, :] = frc_ref[i, pl.ds(t, 1), :]
        h, m, l = pieces(raw[t])
        packed[t, 0:16, :] = h
        packed[t, 16:32, :] = m
        packed[t, 32:48, :] = l
        return carry
    lax.fori_loop(0, tiles, columns, 0, unroll=2)

    def near(t, carry):
        dist = None
        for i in range(3):
            base = t * slots * 8 + (4 if i == 1 else 0)
            chunk = [rows[i // 2, pl.ds(base + r, slots, stride=8), :] for r in range(4)]
            low = jnp.minimum(jnp.minimum(chunk[0], chunk[1]), jnp.minimum(chunk[2], chunk[3]))
            high = jnp.maximum(jnp.maximum(chunk[0], chunk[1]), jnp.maximum(chunk[2], chunk[3]))
            low = jnp.min(low, axis=1, keepdims=True)
            high = jnp.max(high, axis=1, keepdims=True)
            at = pts_ref[i, pl.ds(t, 1), :]
            gap = jnp.maximum(jnp.maximum(low - at, at - high), 0.0)
            dist = gap * gap if dist is None else dist + gap * gap
        mark[pl.ds(pl.multiple_of(t * slots, slots), slots), :] = jnp.where(dist < 1.0001, 1.0, 0.0)
        return carry
    lax.fori_loop(0, tiles, near, 0, unroll=2)

    before = (lax.broadcasted_iota(jnp.int32, (points, points), 0) < lax.broadcasted_iota(jnp.int32, (points, points), 1))
    before = jnp.where(before, 1.0, 0.0).astype(jnp.bfloat16)
    flags = mark[...]
    ones = jnp.ones((16, points), jnp.bfloat16)
    fb = flags.astype(jnp.bfloat16)
    rank = jnp.dot(fb, before, preferred_element_type=jnp.float32)
    spots[...] = jnp.where(flags > 0.5, rank, -1.0)
    sums = lax.dot_general(ones, fb, (((1,), (1,)), ((), ())), preferred_element_type=jnp.float32)
    tally[...] = sums[0:8].astype(jnp.int32)
    cp = pltpu.make_async_copy(tally, count, sem2)
    cp.start()
    cp.wait()

    most = points // ROWS
    def list_pairs(h, m):
        for u in range(slots):
            q = h * slots + u
            for j in range(most):
                jobs[m + j] = q * 16 + j
            m = m + ((count[0, q] + (ROWS - 1)) >> 5)
        return m
    made = lax.fori_loop(0, tiles, list_pairs, 0)
    for u in range(BATCH - 1):
        jobs[made + u] = most
    trips = (made + BATCH - 1) // BATCH

    source = lax.broadcasted_iota(jnp.int32, (48, 6 * 128), 0) & 15
    spread = jnp.where(source == (lax.broadcasted_iota(jnp.int32, (48, 6 * 128), 1) >> 7), 1.0, 0.0).astype(jnp.bfloat16)
    spread_all[...] = spread
    every = jnp.ones((48, 128), jnp.bfloat16)
    lane48 = lax.broadcasted_iota(jnp.int32, (ROWS, 48), 1) & 15
    place32 = lax.broadcasted_iota(jnp.int32, (ROWS, points), 0).astype(jnp.float32)
    lane = lax.broadcasted_iota(jnp.int32, (ROWS, 128), 1)

    def job_of(n):
        job = jobs[n]
        return job >> 4, job & 15

    def bring(first, slot):
        q, j = job_of(first + slot)
        t, k = q // slots, q % slots
        pick = jnp.where(place32 + (j * ROWS).astype(jnp.float32) == spots[pl.ds(q, 1), :], 1.0, 0.0).astype(jnp.bfloat16)
        picks[slot] = pick
        got = lax.dot_general(pick, packed[t], (((1,), (1,)), ((), ())), preferred_element_type=jnp.float32)
        return got.astype(jnp.bfloat16), jnp.where(lane48 == 6 + k, got, 0.0).astype(jnp.bfloat16)

    def work(first, slot):
        q, j = job_of(first + slot)
        px, py, pz, fx, fy, fz, weight = [wide[pl.ds(pl.multiple_of(slot * ROWS, ROWS), ROWS), i * 128:(i + 1) * 128] for i in range(7)]
        shown = [None] * 3
        loads = [[], [], []]
        for g in range(4):
            base = q * 8 + g
            dx = px - rows[0, pl.ds(base, 1), :]
            dy = py - rows[0, pl.ds(base + 4, 1), :]
            dz = pz - rows[1, pl.ds(base, 1), :]
            d2 = jnp.maximum(dx * dx + dy * dy + dz * dz, 1e-30)
            u = jnp.maximum(1.0 - d2 * lax.rsqrt(d2), 0.0)
            u2 = u * u
            val = ((u2 * u2) * weight) * (1.25 - u)
            for i, (pp, off) in enumerate(((1, 4), (2, 0), (2, 4))):
                term = val * rows[pp, pl.ds(base + off, 1), :]
                shown[i] = term if shown[i] is None else shown[i] + term
            for i, f in enumerate((fx, fy, fz)):
                loads[i].append(jnp.sum(val * f, axis=0, keepdims=True))
        for i in range(3):
            moved_sum[slot, i] = shown[i]
        return q, [jnp.concatenate(l, axis=1) for l in loads]

    def give(first, slot):
        q, j = job_of(first + slot)
        cols = [jnp.sum(moved_sum[slot, i], axis=1, keepdims=True) for i in range(3)]
        d = jnp.where(lane == 0, cols[0], jnp.where(lane == 1, cols[1], cols[2]))
        dt = jnp.transpose(d)[0:8]
        dh = dt.astype(jnp.bfloat16)
        dl = (dt - dh.astype(jnp.float32)).astype(jnp.bfloat16)
        back = jnp.dot(jnp.concatenate([dh, dl], axis=0), picks[slot], preferred_element_type=jnp.float32)
        return q // slots, back[0:8] + back[8:16]

    def trip(n, carry):
        first = n * BATCH
        def do_bring(h, c):
            took = [bring(first, h * WIDE + u) for u in range(WIDE)]
            at = pl.ds(pl.multiple_of(h * (WIDE * ROWS), WIDE * ROWS), WIDE * ROWS)
            got = jnp.concatenate([v[0] for v in took], axis=0)
            wide[at, 0:6 * 128] = jnp.dot(got, spread_all[...], preferred_element_type=jnp.float32)
            got = jnp.concatenate([v[1] for v in took], axis=0)
            wide[at, 6 * 128:7 * 128] = jnp.dot(got, every, preferred_element_type=jnp.float32)
            return c
        lax.fori_loop(0, BATCH // WIDE, do_bring, 0)
        def do_work(h, c):
            for q, loads in [work(first, h * UNROLL + u) for u in range(UNROLL)]:
                for i in range(3):
                    part_ref[i, pl.ds(flat[i, q], 1), :] += loads[i]
            return c
        lax.fori_loop(0, BATCH // UNROLL, do_work, 0)
        def do_give(h, c):
            for t, back in [give(first, h * WIDE + u) for u in range(WIDE)]:
                for i in range(3):
                    disp_ref[i, pl.ds(t, 1), :] += back[i:i + 1]
            return c
        lax.fori_loop(0, BATCH // WIDE, do_give, 0)
        return carry
    lax.fori_loop(0, trips, trip, 0)


def pairs(ids, pts, frc, lev, table):
    tiles, slots = ids.shape
    points = pts.shape[-1]
    total = tiles * slots
    clusters = table.shape[1] // 8
    vm = pl.BlockSpec(memory_space=pltpu.VMEM)
    V = lambda s, d=jnp.float32: pltpu.VMEM(s, d)
    return pl.pallas_call(
        pairs_body,
        out_shape=(jax.ShapeDtypeStruct(pts.shape, jnp.float32), jax.ShapeDtypeStruct((3, clusters, 512), jnp.float32)),
        in_specs=[pl.BlockSpec(memory_space=pltpu.SMEM), vm, vm, vm, vm],
        out_specs=(vm, vm),
        scratch_shapes=[
            V((3, total * 8, 128)), V((total, points)), V((tiles, 16, points)), V((tiles, 48, points), jnp.bfloat16),
            V((total, points)), V((BATCH, ROWS, points), jnp.bfloat16), V((BATCH * ROWS, 7 * 128)), V((BATCH, 3, ROWS, 128)),
            V((48, 6 * 128), jnp.bfloat16),
            V((8, total), jnp.int32),
            pltpu.SMEM((3, total), jnp.int32), pltpu.SMEM((total * 8 + BATCH + 8,), jnp.int32), pltpu.SMEM((8, total), jnp.int32),
            pltpu.SemaphoreType.DMA,
        ],
        compiler_params=pltpu.CompilerParams(vmem_limit_bytes=16 * 2**20),
        name="pairs",
    )(ids, pts, frc, lev, table)


def on_device(point_coords, fluid_force, tile_clusters, pu_level, node_coords, node_disp, inverse):
    turn = lambda v: jnp.transpose(v, (1, 0, 2))
    table = all_gather(own_table(turn(node_disp), turn(node_coords), inverse))
    table = table.reshape(3, -1, 128)
    shown, part = pairs(tile_clusters, turn(point_coords), turn(fluid_force), pu_level, table)
    force = reduce_scatter(part.reshape(3, 4, 4, 4, 2, node_coords.shape[0], node_coords.shape[2]))
    return turn(shown), turn(force)


def solution(mesh):
    spec = P(("row", "col"), None, None)
    return jax.shard_map(
        on_device,
        mesh=mesh,
        in_specs=(spec, spec, P(("row", "col"), None), spec, spec, spec, spec),
        out_specs=(spec, spec),
        check_vma=False,
    )
```

```python
import jax
import jax.numpy as jnp
from jax import lax
from jax.experimental import pallas as pl
from jax.experimental.pallas import tpu as pltpu
from jax.sharding import PartitionSpec as P

MESH = pl.DeviceIdType.MESH

def mod4(v):
    return lax.rem(v + 4, 4)

def place():
    row, col = lax.axis_index("row"), lax.axis_index("col")
    return [col // 4, lax.rem(col, 4), row // 2], lax.rem(row, 2)

def device(xyz, core):
    return (xyz[2] * 2 + core, xyz[0] * 4 + xyz[1])

def moved(xyz, dim, by):
    out = list(xyz)
    out[dim] = mod4(out[dim] + by)
    return out

def greet(xyz, core):
    barrier = pltpu.get_barrier_semaphore()
    for dim in range(3):
        for by in (1, -1):
            pl.semaphore_signal(barrier, inc=1, device_id=device(moved(xyz, dim, by), core), device_id_type=MESH)
    pl.semaphore_signal(barrier, inc=1, device_id=device(xyz, 1 - core), device_id_type=MESH)
    pl.semaphore_wait(barrier, 7)

ORDERS = ((0, 1, 2), (1, 2, 0), (2, 0, 1))

def gather_body(own_ref, out_ref, recv, send, near, sib_send, local):
    xyz, core = place()
    greet(xyz, core)
    half = own_ref.shape[1] // 2
    pend = []

    def push(src, dst, to, to_core, rsem, ssem):
        c = pltpu.make_async_remote_copy(src_ref=src, dst_ref=dst, send_sem=ssem, recv_sem=rsem,
                                         device_id=device(to, to_core), device_id_type=MESH)
        c.start()
        pend.append(c)

    def arrive(dst, rsem):
        pltpu.make_async_remote_copy(src_ref=dst, dst_ref=dst, send_sem=rsem, recv_sem=rsem,
                                     device_id=device(xyz, 1 - core), device_id_type=MESH).wait_recv()

    class Part:
        pass
    parts = []
    for p, (a, b, c) in enumerate(ORDERS):
        s = Part()
        s.p, s.a, s.b, s.c = p, a, b, c
        s.ia, s.ib, s.ic = xyz[a], xyz[b], xyz[c]
        s.nsend = 0
        parts.append(s)

    def block(s, ja, jb, jc, sub=None):
        r = out_ref.at[s.p, jc, jb, ja, core]
        return r if sub is None else r.at[sub]

    def group(s, jb, jc, k=None):
        return out_ref.at[s.p, jc, jb, :, core if k is None else k]

    def nsem(s):
        s.nsend += 1
        return send.at[s.p, s.nsend - 1]

    lo, hi = pl.ds(0, half), pl.ds(half, half)
    rel = lambda i, r: mod4(i + r)
    copies = []
    for s in parts:
        own = own_ref.at[s.p]
        cp = pltpu.make_async_copy(own, block(s, s.ia, s.ib, s.ic), local.at[s.p])
        cp.start()
        copies.append(cp)
        for d, by in ((0, 1), (1, -1)):
            push(own, block(s, s.ia, s.ib, s.ic), moved(xyz, s.a, by), core, recv.at[s.p, d], nsem(s))
    for s in parts:
        own = own_ref.at[s.p]
        for d, by in ((0, 1), (1, -1)):
            push(own, block(s, s.ia, s.ib, s.ic), moved(xyz, s.b, by), core, recv.at[s.p, 4 + 4 * d + 0], nsem(s))

    def send_b(s, r):
        ja = rel(s.ia, r)
        for d, by in ((0, 1), (1, -1)):
            push(block(s, ja, s.ib, s.ic), block(s, ja, s.ib, s.ic), moved(xyz, s.b, by), core,
                 recv.at[s.p, 4 + 4 * d + r], nsem(s))

    for s in parts:
        ja = rel(s.ia, -1)
        arrive(block(s, ja, s.ib, s.ic), recv.at[s.p, 0])
        push(block(s, ja, s.ib, s.ic, lo), block(s, ja, s.ib, s.ic, lo), moved(xyz, s.a, 1), core, recv.at[s.p, 2], nsem(s))
        ja2 = rel(s.ia, 1)
        arrive(block(s, ja2, s.ib, s.ic), recv.at[s.p, 1])
        push(block(s, ja2, s.ib, s.ic, hi), block(s, ja2, s.ib, s.ic, hi), moved(xyz, s.a, -1), core, recv.at[s.p, 3], nsem(s))
        send_b(s, 3)
        send_b(s, 1)

    def sib(s, jb, jc, slot):
        push(group(s, jb, jc), group(s, jb, jc), xyz, 1 - core, near.at[s.p, slot], sib_send.at[s.p, slot])

    def send_c(s, r):
        jb = rel(s.ib, r)
        for d, by in ((0, 1), (1, -1)):
            push(group(s, jb, s.ic), group(s, jb, s.ic), moved(xyz, s.c, by), core,
                 recv.at[s.p, 16 + 4 * d + r], nsem(s))
        sib(s, jb, s.ic, r)

    for s, cp in zip(parts, copies):
        ja = rel(s.ia, 2)
        arrive(block(s, ja, s.ib, s.ic, lo), recv.at[s.p, 2])
        arrive(block(s, ja, s.ib, s.ic, hi), recv.at[s.p, 3])
        send_b(s, 2)
        cp.wait()
        send_c(s, 0)
    for s in parts:
        for r in (0, 3, 1, 2):
            ja = rel(s.ia, r)
            for d, by in ((0, 1), (1, -1)):
                jb = rel(s.ib, -by)
                arrive(block(s, ja, jb, s.ic), recv.at[s.p, 4 + 4 * d + r])
                if (d == 0) == (r in (0, 3)):
                    push(block(s, ja, jb, s.ic), block(s, ja, jb, s.ic), moved(xyz, s.b, by), core,
                         recv.at[s.p, 12 + r], nsem(s))
        send_c(s, 3)
        send_c(s, 1)
    for s in parts:
        jb = rel(s.ib, 2)
        for r in (0, 3, 1, 2):
            arrive(block(s, rel(s.ia, r), jb, s.ic), recv.at[s.p, 12 + r])
        send_c(s, 2)
    for r in (0, 3, 1, 2):
        for s in parts:
            jb = rel(s.ib, r)
            for d, by in ((0, 1), (1, -1)):
                jc = rel(s.ic, -by)
                arrive(group(s, jb, jc), recv.at[s.p, 16 + 4 * d + r])
                if (d == 0) == (r in (0, 3)):
                    push(group(s, jb, jc), group(s, jb, jc), moved(xyz, s.c, by), core, recv.at[s.p, 24 + r], nsem(s))
                sib(s, jb, jc, 4 + 4 * d + r)
    for r in (0, 3, 1, 2):
        for s in parts:
            jb, jc = rel(s.ib, r), rel(s.ic, 2)
            arrive(group(s, jb, jc), recv.at[s.p, 24 + r])
            sib(s, jb, jc, 12 + r)
    for s in parts:
        for r in range(4):
            for slot, jc in ((r, s.ic), (4 + r, rel(s.ic, -1)), (8 + r, rel(s.ic, 1)), (12 + r, rel(s.ic, 2))):
                arrive(group(s, rel(s.ib, r), jc, 1 - core), near.at[s.p, slot])
    for c in pend:
        c.wait_send()

def all_gather(own):
    parts, clusters, rows, lanes = own.shape
    return pl.pallas_call(
        gather_body,
        out_shape=jax.ShapeDtypeStruct((parts, 4, 4, 4, 2, clusters, rows, lanes), jnp.float32),
        in_specs=[pl.BlockSpec(memory_space=pltpu.VMEM)],
        out_specs=pl.BlockSpec(memory_space=pltpu.VMEM),
        scratch_shapes=[
            pltpu.SemaphoreType.DMA((3, 28)),
            pltpu.SemaphoreType.DMA((3, 28)),
            pltpu.SemaphoreType.DMA((3, 16)),
            pltpu.SemaphoreType.DMA((3, 16)),
            pltpu.SemaphoreType.DMA((3,)),
        ],
        compiler_params=pltpu.CompilerParams(collective_id=0, has_side_effects=True, vmem_limit_bytes=2 * 2**20),
        name="torus_gather",
    )(own)


FIRST = (2, 3, 1, 0)
UP, DOWN = (2, 1), (3, 0)

def scatter_body(part_ref, out_ref, held, other, in_c, in_b, far_a, in_a,
                 near, near_send, rc, sc, rb, sb, ra, sa):
    xyz, core = place()
    pend = []
    rel = lambda i, r: mod4(i + r)
    info = []
    for p, (a, b, c) in enumerate(ORDERS):
        info.append((p, a, b, c, xyz[a], xyz[b], xyz[c]))

    def push(src, dst, to, to_core, rsem, ssem):
        cp = pltpu.make_async_remote_copy(src_ref=src, dst_ref=dst, send_sem=ssem, recv_sem=rsem,
                                          device_id=device(to, to_core), device_id_type=MESH)
        cp.start()
        pend.append(cp)

    def arrive(dst, rsem):
        pltpu.make_async_remote_copy(src_ref=dst, dst_ref=dst, send_sem=rsem, recv_sem=rsem,
                                     device_id=device(xyz, 1 - core), device_id_type=MESH).wait_recv()

    def swap(r4):
        for r in FIRST:
            for p, a, b, c, ia, ib, ic in info:
                jc, jb = rel(ic, r4), rel(ib, r)
                push(part_ref.at[p, jc, jb, :, 1 - core], other.at[p, jc, jb], xyz, 1 - core,
                     near.at[p, r4 * 4 + r], near_send.at[p, r4 * 4 + r])
    greet(xyz, core)
    for r4 in (2, 1, 3, 0):
        swap(r4)

    def ready(p, r4, r, jc, jb):
        arrive(other.at[p, jc, jb], near.at[p, r4 * 4 + r])

    for r in FIRST:
        for p, a, b, c, ia, ib, ic in info:
            jc, jb = rel(ic, 2), rel(ib, r)
            ready(p, 2, r, jc, jb)
            held[p, jc, jb] = part_ref[p, jc, jb, :, core] + other[p, jc, jb]
            push(held.at[p, jc, jb], in_c.at[p, r], moved(xyz, c, 1 if r in UP else -1), core, rc.at[p, r], sc.at[p, r])
    for up, r, far in ((True, 3, False), (False, 2, False), (True, 0, False), (False, 1, False),
                       (True, 2, True), (False, 3, True), (True, 1, True), (False, 0, True)):
        for p, a, b, c, ia, ib, ic in info:
            by = 1 if up else -1
            jc, jb = rel(ic, by), rel(ib, r)
            ready(p, 1 if up else 3, r, jc, jb)
            if far:
                arrive(in_c.at[p, r], rc.at[p, r])
                held[p, jc, jb] = part_ref[p, jc, jb, :, core] + other[p, jc, jb] + in_c[p, r]
            else:
                held[p, jc, jb] = part_ref[p, jc, jb, :, core] + other[p, jc, jb]
            slot = (4 if up else 8) + r
            push(held.at[p, jc, jb], in_c.at[p, slot], moved(xyz, c, by), core, rc.at[p, slot], sc.at[p, slot])
    def finish_c(r):
        for p, a, b, c, ia, ib, ic in info:
            jc, jb = ic, rel(ib, r)
            ready(p, 0, r, jc, jb)
            arrive(in_c.at[p, 4 + r], rc.at[p, 4 + r])
            arrive(in_c.at[p, 8 + r], rc.at[p, 8 + r])
            held[p, jc, jb] = part_ref[p, jc, jb, :, core] + other[p, jc, jb] + (in_c[p, 4 + r] + in_c[p, 8 + r])
    def send_b(p, b, jc, jb, ja, slot, by):
        push(held.at[p, jc, jb, ja], in_b.at[p, slot], moved(xyz, b, by), core, rb.at[p, slot], sb.at[p, slot])
    finish_c(2)
    for q in FIRST:
        for p, a, b, c, ia, ib, ic in info:
            send_b(p, b, ic, rel(ib, 2), rel(ia, q), q, 1 if q in UP else -1)
    finish_c(3)
    finish_c(1)
    for q in (3, 0):
        for p, a, b, c, ia, ib, ic in info:
            send_b(p, b, ic, rel(ib, 1), rel(ia, q), 4 + q, 1)
    for q in (2, 1):
        for p, a, b, c, ia, ib, ic in info:
            send_b(p, b, ic, rel(ib, 3), rel(ia, q), 8 + q, -1)
    for up, q in ((True, 2), (False, 3), (True, 1), (False, 0)):
        for p, a, b, c, ia, ib, ic in info:
            by = 1 if up else -1
            jc, jb, ja = ic, rel(ib, by), rel(ia, q)
            arrive(in_b.at[p, q], rb.at[p, q])
            held[p, jc, jb, ja] = held[p, jc, jb, ja] + in_b[p, q]
            send_b(p, b, jc, jb, ja, (4 if up else 8) + q, by)
    finish_c(0)
    def finish_b(q):
        for p, a, b, c, ia, ib, ic in info:
            ja = rel(ia, q)
            arrive(in_b.at[p, 4 + q], rb.at[p, 4 + q])
            arrive(in_b.at[p, 8 + q], rb.at[p, 8 + q])
            held[p, ic, ib, ja] = held[p, ic, ib, ja] + (in_b[p, 4 + q] + in_b[p, 8 + q])
    finish_b(2)
    lo, hi = pl.ds(0, 8), pl.ds(8, 8)
    for p, a, b, c, ia, ib, ic in info:
        blk = held.at[p, ic, ib, rel(ia, 2)]
        push(blk.at[lo], far_a.at[p, 0], moved(xyz, a, 1), core, ra.at[p, 0], sa.at[p, 0])
        push(blk.at[hi], far_a.at[p, 1], moved(xyz, a, -1), core, ra.at[p, 1], sa.at[p, 1])
    finish_b(1)
    finish_b(3)
    for p, a, b, c, ia, ib, ic in info:
        ja = rel(ia, 1)
        arrive(far_a.at[p, 0], ra.at[p, 0])
        held[p, ic, ib, ja, 0:8] = held[p, ic, ib, ja, 0:8] + far_a[p, 0]
        push(held.at[p, ic, ib, ja], in_a.at[p, 0], moved(xyz, a, 1), core, ra.at[p, 2], sa.at[p, 2])
        ja = rel(ia, 3)
        arrive(far_a.at[p, 1], ra.at[p, 1])
        held[p, ic, ib, ja, 8:16] = held[p, ic, ib, ja, 8:16] + far_a[p, 1]
        push(held.at[p, ic, ib, ja], in_a.at[p, 1], moved(xyz, a, -1), core, ra.at[p, 3], sa.at[p, 3])
    finish_b(0)
    for p, a, b, c, ia, ib, ic in info:
        arrive(in_a.at[p, 0], ra.at[p, 2])
        arrive(in_a.at[p, 1], ra.at[p, 3])
        out_ref[p] = held[p, ic, ib, ia] + (in_a[p, 0] + in_a[p, 1])
    for cp in pend:
        cp.wait_send()

def reduce_scatter(part):
    clusters, nodes = part.shape[-2:]
    D = pltpu.SemaphoreType.DMA
    V = lambda *s: pltpu.VMEM(s + (clusters, nodes), jnp.float32)
    return pl.pallas_call(
        scatter_body,
        out_shape=jax.ShapeDtypeStruct((3, clusters, nodes), jnp.float32),
        in_specs=[pl.BlockSpec(memory_space=pltpu.VMEM)],
        out_specs=pl.BlockSpec(memory_space=pltpu.VMEM),
        scratch_shapes=[V(3, 4, 4, 4), V(3, 4, 4, 4), V(3, 12, 4), V(3, 12),
                        pltpu.VMEM((3, 2, clusters // 2, nodes), jnp.float32), V(3, 2),
                        D((3, 16)), D((3, 16)), D((3, 12)), D((3, 12)), D((3, 12)), D((3, 12)),
                        D((3, 4)), D((3, 4))],
        compiler_params=pltpu.CompilerParams(collective_id=1, has_side_effects=True, vmem_limit_bytes=24 * 2**20),
        name="torus_scatter",
    )(part)

ROWS = 32
GROUP = 2
BATCH = 8

def pieces(value):
    high = value.astype(jnp.bfloat16)
    rest = value - high.astype(jnp.float32)
    mid = rest.astype(jnp.bfloat16)
    low = (rest - mid.astype(jnp.float32)).astype(jnp.bfloat16)
    return high, mid, low


def coeff_body(disp_ref, coords_ref, inverse_ref, table_ref):
    nodes = inverse_ref.shape[-1]
    for u in range(GROUP):
        c = pl.program_id(0) * GROUP + u
        left = jnp.concatenate([disp_ref[i, pl.ds(c, 1), :] for i in range(3)] + [jnp.zeros((5, nodes), jnp.float32)], axis=0)
        lh = left.astype(jnp.bfloat16)
        ll = (left - lh.astype(jnp.float32)).astype(jnp.bfloat16)
        both = jnp.concatenate([lh, ll], axis=0)
        whole = inverse_ref[u]
        ih = whole.astype(jnp.bfloat16)
        il = (whole - ih.astype(jnp.float32)).astype(jnp.bfloat16)
        top = jnp.dot(both, ih, preferred_element_type=jnp.float32)
        low = jnp.dot(both, il, preferred_element_type=jnp.float32)
        res = top[0:8] + (top[8:16] + low[0:8])
        for i in range(6):
            row = coords_ref[i, pl.ds(c, 1), :] if i < 3 else res[i - 3:i - 2]
            for q in range(4):
                table_ref[i // 2, c, pl.ds((i % 2) * 4 + q, 1), :] = row[:, q * 128:(q + 1) * 128]


def own_table(node_disp, node_coords, inverse):
    clusters, nodes = inverse.shape[0], inverse.shape[1]
    whole = pl.BlockSpec((3, clusters, nodes), lambda c: (0, 0, 0))
    return pl.pallas_call(
        coeff_body,
        grid=(clusters // GROUP,),
        out_shape=jax.ShapeDtypeStruct((3, clusters, 8, 128), jnp.float32),
        in_specs=[whole, whole, pl.BlockSpec((GROUP, nodes, nodes), lambda c: (c, 0, 0))],
        out_specs=pl.BlockSpec((3, clusters, 8, 128), lambda c: (0, 0, 0, 0)),
        name="coefficients",
    )(node_disp, node_coords, inverse)


def pairs_body(ids_ref, pts_ref, frc_ref, lev_ref, table_ref, disp_ref, part_ref,
               rows, spots, raw, packed, mark, wide_a, wide_b, sums_a, sums_b, spread_all, tally, flat, jobs, count, sem2):
    tiles, slots = ids_ref.shape
    points = pts_ref.shape[-1]
    total = tiles * slots

    def fetch(t, carry):
        for k in range(slots):
            cid = ids_ref[t, k]
            l, dev = cid & 15, cid >> 4
            core, z = (dev >> 4) & 1, dev >> 5
            y, x = dev & 3, (dev >> 2) & 3
            for p, (a, b, c) in enumerate(((x, y, z), (y, z, x), (z, x, y))):
                f = (((c * 4 + b) * 4 + a) * 2 + core) * 16 + l
                flat[p, t * slots + k] = f
                rows[p, pl.ds(pl.multiple_of((t * slots + k) * 8, 8), 8), :] = table_ref[p, pl.ds(pl.multiple_of(f * 8, 8), 8), :]
        return carry
    lax.fori_loop(0, tiles, fetch, 0)

    def clear(g, carry):
        part_ref[0, pl.ds(pl.multiple_of(g * 16, 16), 16), :] = jnp.zeros((16, part_ref.shape[2]), jnp.float32)
        part_ref[1, pl.ds(pl.multiple_of(g * 16, 16), 16), :] = jnp.zeros((16, part_ref.shape[2]), jnp.float32)
        part_ref[2, pl.ds(pl.multiple_of(g * 16, 16), 16), :] = jnp.zeros((16, part_ref.shape[2]), jnp.float32)
        return carry
    lax.fori_loop(0, part_ref.shape[1] // 16, clear, 0)
    disp_ref[...] = jnp.zeros(disp_ref.shape, jnp.float32)

    def columns(t, carry):
        level = lev_ref[t].astype(jnp.float32) + 1.0
        weight = level / jnp.sum(level, axis=0, keepdims=True)
        raw[t, 6:14, :] = weight * 4.0
        raw[t, 14:16, :] = jnp.zeros((2, points), jnp.float32)
        for i in range(3):
            raw[t, i:i + 1, :] = pts_ref[i, pl.ds(t, 1), :]
            raw[t, 3 + i:4 + i, :] = frc_ref[i, pl.ds(t, 1), :]
        h, m, l = pieces(raw[t])
        packed[t, 0:16, :] = h
        packed[t, 16:32, :] = m
        packed[t, 32:48, :] = l
        return carry
    lax.fori_loop(0, tiles, columns, 0, unroll=2)

    def near(t, carry):
        dist = None
        for i in range(3):
            base = t * slots * 8 + (4 if i == 1 else 0)
            chunk = [rows[i // 2, pl.ds(base + r, slots, stride=8), :] for r in range(4)]
            low = jnp.minimum(jnp.minimum(chunk[0], chunk[1]), jnp.minimum(chunk[2], chunk[3]))
            high = jnp.maximum(jnp.maximum(chunk[0], chunk[1]), jnp.maximum(chunk[2], chunk[3]))
            low = jnp.min(low, axis=1, keepdims=True)
            high = jnp.max(high, axis=1, keepdims=True)
            at = pts_ref[i, pl.ds(t, 1), :]
            gap = jnp.maximum(jnp.maximum(low - at, at - high), 0.0)
            dist = gap * gap if dist is None else dist + gap * gap
        mark[pl.ds(pl.multiple_of(t * slots, slots), slots), :] = jnp.where(dist < 1.0001, 1.0, 0.0)
        return carry
    lax.fori_loop(0, tiles, near, 0, unroll=2)

    before = (lax.broadcasted_iota(jnp.int32, (points, points), 0) < lax.broadcasted_iota(jnp.int32, (points, points), 1))
    before = jnp.where(before, 1.0, 0.0).astype(jnp.bfloat16)
    flags = mark[...]
    ones = jnp.ones((16, points), jnp.bfloat16)
    fb = flags.astype(jnp.bfloat16)
    rank = jnp.dot(fb, before, preferred_element_type=jnp.float32)
    spots[...] = jnp.where(flags > 0.5, rank, -1.0)
    sums = lax.dot_general(ones, fb, (((1,), (1,)), ((), ())), preferred_element_type=jnp.float32)
    tally[...] = sums[0:8].astype(jnp.int32)
    cp = pltpu.make_async_copy(tally, count, sem2)
    cp.start()
    cp.wait()

    most = points // ROWS
    def list_pairs(h, m):
        for u in range(slots):
            q = h * slots + u
            for j in range(most):
                jobs[m + j] = q * 16 + j
            m = m + ((count[0, q] + (ROWS - 1)) >> 5)
        return m
    for u in range(BATCH):
        jobs[u] = most
    made = lax.fori_loop(0, tiles, list_pairs, BATCH)
    for u in range(4 * BATCH):
        jobs[made + u] = most
    trips = (made - BATCH + 2 * BATCH - 1) // (2 * BATCH)

    source = lax.broadcasted_iota(jnp.int32, (48, 6 * 128), 0) & 15
    spread = jnp.where(source == (lax.broadcasted_iota(jnp.int32, (48, 6 * 128), 1) >> 7), 1.0, 0.0).astype(jnp.bfloat16)
    spread_all[...] = spread
    every = jnp.ones((48, 128), jnp.bfloat16)
    lane48 = lax.broadcasted_iota(jnp.int32, (ROWS, 48), 1) & 15
    place32 = lax.broadcasted_iota(jnp.int32, (ROWS, points), 0).astype(jnp.float32)
    lane = lax.broadcasted_iota(jnp.int32, (ROWS, 128), 1)

    def pick_of(job):
        q, j = job >> 4, job & 15
        return q, jnp.where(place32 + (j * ROWS).astype(jnp.float32) == spots[pl.ds(q, 1), :], 1.0, 0.0).astype(jnp.bfloat16)

    def bring(batch, wide):
        plain, chosen = [], []
        for u in range(BATCH):
            q, pick = pick_of(jobs[(batch + 1) * BATCH + u])
            got = lax.dot_general(pick, packed[q // slots], (((1,), (1,)), ((), ())), preferred_element_type=jnp.float32)
            plain.append(got.astype(jnp.bfloat16))
            chosen.append(jnp.where(lane48 == 6 + q % slots, got, 0.0).astype(jnp.bfloat16))
        wide[:, 0:6 * 128] = jnp.dot(jnp.concatenate(plain, axis=0), spread_all[...], preferred_element_type=jnp.float32)
        wide[:, 6 * 128:7 * 128] = jnp.dot(jnp.concatenate(chosen, axis=0), every, preferred_element_type=jnp.float32)

    def work(batch, wide, sums):
        for slot in range(BATCH):
            q = jobs[(batch + 1) * BATCH + slot] >> 4
            px, py, pz, fx, fy, fz, weight = [wide[slot * ROWS:(slot + 1) * ROWS, i * 128:(i + 1) * 128] for i in range(7)]
            shown = [None] * 3
            loads = [[], [], []]
            for g in range(4):
                base = q * 8 + g
                dx = px - rows[0, pl.ds(base, 1), :]
                dy = py - rows[0, pl.ds(base + 4, 1), :]
                dz = pz - rows[1, pl.ds(base, 1), :]
                d2 = jnp.maximum(dx * dx + dy * dy + dz * dz, 1e-30)
                u = jnp.maximum(1.0 - d2 * lax.rsqrt(d2), 0.0)
                u2 = u * u
                val = ((u2 * u2) * weight) * (1.25 - u)
                for i, (pp, off) in enumerate(((1, 4), (2, 0), (2, 4))):
                    term = val * rows[pp, pl.ds(base + off, 1), :]
                    shown[i] = term if shown[i] is None else shown[i] + term
                for i, f in enumerate((fx, fy, fz)):
                    loads[i].append(jnp.sum(val * f, axis=0, keepdims=True))
            for i in range(3):
                sums[slot, i] = shown[i]
                part_ref[i, pl.ds(flat[i, q], 1), :] += jnp.concatenate(loads[i], axis=1)

    def give(batch, sums):
        backs = []
        for slot in range(BATCH):
            q, pick = pick_of(jobs[(batch + 1) * BATCH + slot])
            cols = [jnp.sum(sums[slot, i], axis=1, keepdims=True) for i in range(3)]
            d = jnp.where(lane == 0, cols[0], jnp.where(lane == 1, cols[1], cols[2]))
            dt = jnp.transpose(d)[0:8]
            dh = dt.astype(jnp.bfloat16)
            dl = (dt - dh.astype(jnp.float32)).astype(jnp.bfloat16)
            back = jnp.dot(jnp.concatenate([dh, dl], axis=0), pick, preferred_element_type=jnp.float32)
            backs.append((q // slots, back[0:8] + back[8:16]))
        for t, back in backs:
            for i in range(3):
                disp_ref[i, pl.ds(t, 1), :] += back[i:i + 1]

    sums_b[...] = jnp.zeros(sums_b.shape, jnp.float32)
    bring(0, wide_a)

    def trip(n, carry):
        bring(2 * n + 1, wide_b)
        work(2 * n, wide_a, sums_a)
        give(2 * n - 1, sums_b)
        bring(2 * n + 2, wide_a)
        work(2 * n + 1, wide_b, sums_b)
        give(2 * n, sums_a)
        return carry
    lax.fori_loop(0, trips, trip, 0)
    give(2 * trips - 1, sums_b)


def pairs(ids, pts, frc, lev, table):
    tiles, slots = ids.shape
    points = pts.shape[-1]
    total = tiles * slots
    clusters = table.shape[1] // 8
    vm = pl.BlockSpec(memory_space=pltpu.VMEM)
    V = lambda s, d=jnp.float32: pltpu.VMEM(s, d)
    return pl.pallas_call(
        pairs_body,
        out_shape=(jax.ShapeDtypeStruct(pts.shape, jnp.float32), jax.ShapeDtypeStruct((3, clusters, 512), jnp.float32)),
        in_specs=[pl.BlockSpec(memory_space=pltpu.SMEM), vm, vm, vm, vm],
        out_specs=(vm, vm),
        scratch_shapes=[
            V((3, total * 8, 128)), V((total, points)), V((tiles, 16, points)), V((tiles, 48, points), jnp.bfloat16),
            V((total, points)), V((BATCH * ROWS, 7 * 128)), V((BATCH * ROWS, 7 * 128)),
            V((BATCH, 3, ROWS, 128)), V((BATCH, 3, ROWS, 128)),
            V((48, 6 * 128), jnp.bfloat16),
            V((8, total), jnp.int32),
            pltpu.SMEM((3, total), jnp.int32), pltpu.SMEM((total * 8 + 5 * BATCH + 8,), jnp.int32), pltpu.SMEM((8, total), jnp.int32),
            pltpu.SemaphoreType.DMA,
        ],
        compiler_params=pltpu.CompilerParams(vmem_limit_bytes=16 * 2**20),
        name="pairs",
    )(ids, pts, frc, lev, table)


def on_device(point_coords, fluid_force, tile_clusters, pu_level, node_coords, node_disp, inverse):
    turn = lambda v: jnp.transpose(v, (1, 0, 2))
    table = all_gather(own_table(turn(node_disp), turn(node_coords), inverse))
    table = table.reshape(3, -1, 128)
    shown, part = pairs(tile_clusters, turn(point_coords), turn(fluid_force), pu_level, table)
    force = reduce_scatter(part.reshape(3, 4, 4, 4, 2, node_coords.shape[0], node_coords.shape[2]))
    return turn(shown), turn(force)


def solution(mesh):
    spec = P(("row", "col"), None, None)
    return jax.shard_map(
        on_device,
        mesh=mesh,
        in_specs=(spec, spec, P(("row", "col"), None), spec, spec, spec, spec),
        out_specs=(spec, spec),
        check_vma=False,
    )
```

```python
import jax
import jax.numpy as jnp
from jax import lax
from jax.experimental import pallas as pl
from jax.experimental.pallas import tpu as pltpu
from jax.sharding import PartitionSpec as P

MESH = pl.DeviceIdType.MESH

def mod4(v):
    return lax.rem(v + 4, 4)

def place():
    row, col = lax.axis_index("row"), lax.axis_index("col")
    return [col // 4, lax.rem(col, 4), row // 2], lax.rem(row, 2)

def device(xyz, core):
    return (xyz[2] * 2 + core, xyz[0] * 4 + xyz[1])

def moved(xyz, dim, by):
    out = list(xyz)
    out[dim] = mod4(out[dim] + by)
    return out

def greet(xyz, core):
    barrier = pltpu.get_barrier_semaphore()
    for dim in range(3):
        for by in (1, -1):
            pl.semaphore_signal(barrier, inc=1, device_id=device(moved(xyz, dim, by), core), device_id_type=MESH)
    pl.semaphore_signal(barrier, inc=1, device_id=device(xyz, 1 - core), device_id_type=MESH)
    pl.semaphore_wait(barrier, 7)

ORDERS = ((0, 1, 2), (1, 2, 0), (2, 0, 1))

def gather_body(own_ref, out_ref, recv, send, near, sib_send, local):
    xyz, core = place()
    greet(xyz, core)
    half = own_ref.shape[1] // 2
    pend = []

    def push(src, dst, to, to_core, rsem, ssem):
        c = pltpu.make_async_remote_copy(src_ref=src, dst_ref=dst, send_sem=ssem, recv_sem=rsem,
                                         device_id=device(to, to_core), device_id_type=MESH)
        c.start()
        pend.append(c)

    def arrive(dst, rsem):
        pltpu.make_async_remote_copy(src_ref=dst, dst_ref=dst, send_sem=rsem, recv_sem=rsem,
                                     device_id=device(xyz, 1 - core), device_id_type=MESH).wait_recv()

    class Part:
        pass
    parts = []
    for p, (a, b, c) in enumerate(ORDERS):
        s = Part()
        s.p, s.a, s.b, s.c = p, a, b, c
        s.ia, s.ib, s.ic = xyz[a], xyz[b], xyz[c]
        s.nsend = 0
        parts.append(s)

    def block(s, ja, jb, jc, sub=None):
        r = out_ref.at[s.p, jc, jb, ja, core]
        return r if sub is None else r.at[sub]

    def group(s, jb, jc, k=None):
        return out_ref.at[s.p, jc, jb, :, core if k is None else k]

    def nsem(s):
        s.nsend += 1
        return send.at[s.p, s.nsend - 1]

    lo, hi = pl.ds(0, half), pl.ds(half, half)
    rel = lambda i, r: mod4(i + r)
    copies = []
    for s in parts:
        own = own_ref.at[s.p]
        cp = pltpu.make_async_copy(own, block(s, s.ia, s.ib, s.ic), local.at[s.p])
        cp.start()
        copies.append(cp)
        for d, by in ((0, 1), (1, -1)):
            push(own, block(s, s.ia, s.ib, s.ic), moved(xyz, s.a, by), core, recv.at[s.p, d], nsem(s))
    for s in parts:
        own = own_ref.at[s.p]
        for d, by in ((0, 1), (1, -1)):
            push(own, block(s, s.ia, s.ib, s.ic), moved(xyz, s.b, by), core, recv.at[s.p, 4 + 4 * d + 0], nsem(s))

    def send_b(s, r):
        ja = rel(s.ia, r)
        for d, by in ((0, 1), (1, -1)):
            push(block(s, ja, s.ib, s.ic), block(s, ja, s.ib, s.ic), moved(xyz, s.b, by), core,
                 recv.at[s.p, 4 + 4 * d + r], nsem(s))

    for s in parts:
        ja = rel(s.ia, -1)
        arrive(block(s, ja, s.ib, s.ic), recv.at[s.p, 0])
        push(block(s, ja, s.ib, s.ic, lo), block(s, ja, s.ib, s.ic, lo), moved(xyz, s.a, 1), core, recv.at[s.p, 2], nsem(s))
        ja2 = rel(s.ia, 1)
        arrive(block(s, ja2, s.ib, s.ic), recv.at[s.p, 1])
        push(block(s, ja2, s.ib, s.ic, hi), block(s, ja2, s.ib, s.ic, hi), moved(xyz, s.a, -1), core, recv.at[s.p, 3], nsem(s))
        send_b(s, 3)
        send_b(s, 1)

    def sib(s, jb, jc, slot):
        push(group(s, jb, jc), group(s, jb, jc), xyz, 1 - core, near.at[s.p, slot], sib_send.at[s.p, slot])

    def send_c(s, r):
        jb = rel(s.ib, r)
        for d, by in ((0, 1), (1, -1)):
            push(group(s, jb, s.ic), group(s, jb, s.ic), moved(xyz, s.c, by), core,
                 recv.at[s.p, 16 + 4 * d + r], nsem(s))
        sib(s, jb, s.ic, r)

    for s, cp in zip(parts, copies):
        ja = rel(s.ia, 2)
        arrive(block(s, ja, s.ib, s.ic, lo), recv.at[s.p, 2])
        arrive(block(s, ja, s.ib, s.ic, hi), recv.at[s.p, 3])
        send_b(s, 2)
        cp.wait()
        send_c(s, 0)
    for s in parts:
        for r in (0, 3, 1, 2):
            ja = rel(s.ia, r)
            for d, by in ((0, 1), (1, -1)):
                jb = rel(s.ib, -by)
                arrive(block(s, ja, jb, s.ic), recv.at[s.p, 4 + 4 * d + r])
                if (d == 0) == (r in (0, 3)):
                    push(block(s, ja, jb, s.ic), block(s, ja, jb, s.ic), moved(xyz, s.b, by), core,
                         recv.at[s.p, 12 + r], nsem(s))
        send_c(s, 3)
        send_c(s, 1)
    for s in parts:
        jb = rel(s.ib, 2)
        for r in (0, 3, 1, 2):
            arrive(block(s, rel(s.ia, r), jb, s.ic), recv.at[s.p, 12 + r])
        send_c(s, 2)
    for r in (0, 3, 1, 2):
        for s in parts:
            jb = rel(s.ib, r)
            for d, by in ((0, 1), (1, -1)):
                jc = rel(s.ic, -by)
                arrive(group(s, jb, jc), recv.at[s.p, 16 + 4 * d + r])
                if (d == 0) == (r in (0, 3)):
                    push(group(s, jb, jc), group(s, jb, jc), moved(xyz, s.c, by), core, recv.at[s.p, 24 + r], nsem(s))
                sib(s, jb, jc, 4 + 4 * d + r)
    for r in (0, 3, 1, 2):
        for s in parts:
            jb, jc = rel(s.ib, r), rel(s.ic, 2)
            arrive(group(s, jb, jc), recv.at[s.p, 24 + r])
            sib(s, jb, jc, 12 + r)
    for s in parts:
        for r in range(4):
            for slot, jc in ((r, s.ic), (4 + r, rel(s.ic, -1)), (8 + r, rel(s.ic, 1)), (12 + r, rel(s.ic, 2))):
                arrive(group(s, rel(s.ib, r), jc, 1 - core), near.at[s.p, slot])
    for c in pend:
        c.wait_send()

def all_gather(own):
    parts, clusters, rows, lanes = own.shape
    return pl.pallas_call(
        gather_body,
        out_shape=jax.ShapeDtypeStruct((parts, 4, 4, 4, 2, clusters, rows, lanes), jnp.float32),
        in_specs=[pl.BlockSpec(memory_space=pltpu.VMEM)],
        out_specs=pl.BlockSpec(memory_space=pltpu.VMEM),
        scratch_shapes=[
            pltpu.SemaphoreType.DMA((3, 28)),
            pltpu.SemaphoreType.DMA((3, 28)),
            pltpu.SemaphoreType.DMA((3, 16)),
            pltpu.SemaphoreType.DMA((3, 16)),
            pltpu.SemaphoreType.DMA((3,)),
        ],
        compiler_params=pltpu.CompilerParams(collective_id=0, has_side_effects=True, vmem_limit_bytes=2 * 2**20),
        name="torus_gather",
    )(own)


FIRST = (2, 3, 1, 0)
UP, DOWN = (2, 1), (3, 0)

def scatter_body(part_ref, out_ref, held, other, in_c, in_b, far_a, in_a,
                 near, near_send, rc, sc, rb, sb, ra, sa):
    xyz, core = place()
    pend = []
    rel = lambda i, r: mod4(i + r)
    info = []
    for p, (a, b, c) in enumerate(ORDERS):
        info.append((p, a, b, c, xyz[a], xyz[b], xyz[c]))

    def push(src, dst, to, to_core, rsem, ssem):
        cp = pltpu.make_async_remote_copy(src_ref=src, dst_ref=dst, send_sem=ssem, recv_sem=rsem,
                                          device_id=device(to, to_core), device_id_type=MESH)
        cp.start()
        pend.append(cp)

    def arrive(dst, rsem):
        pltpu.make_async_remote_copy(src_ref=dst, dst_ref=dst, send_sem=rsem, recv_sem=rsem,
                                     device_id=device(xyz, 1 - core), device_id_type=MESH).wait_recv()

    def swap(r4):
        for r in FIRST:
            for p, a, b, c, ia, ib, ic in info:
                jc, jb = rel(ic, r4), rel(ib, r)
                push(part_ref.at[p, jc, jb, :, 1 - core], other.at[p, jc, jb], xyz, 1 - core,
                     near.at[p, r4 * 4 + r], near_send.at[p, r4 * 4 + r])
    greet(xyz, core)
    for r4 in (2, 1, 3, 0):
        swap(r4)

    def ready(p, r4, r, jc, jb):
        arrive(other.at[p, jc, jb], near.at[p, r4 * 4 + r])

    for r in FIRST:
        for p, a, b, c, ia, ib, ic in info:
            jc, jb = rel(ic, 2), rel(ib, r)
            ready(p, 2, r, jc, jb)
            held[p, jc, jb] = part_ref[p, jc, jb, :, core] + other[p, jc, jb]
            push(held.at[p, jc, jb], in_c.at[p, r], moved(xyz, c, 1 if r in UP else -1), core, rc.at[p, r], sc.at[p, r])
    for up, r, far in ((True, 3, False), (False, 2, False), (True, 0, False), (False, 1, False),
                       (True, 2, True), (False, 3, True), (True, 1, True), (False, 0, True)):
        for p, a, b, c, ia, ib, ic in info:
            by = 1 if up else -1
            jc, jb = rel(ic, by), rel(ib, r)
            ready(p, 1 if up else 3, r, jc, jb)
            if far:
                arrive(in_c.at[p, r], rc.at[p, r])
                held[p, jc, jb] = part_ref[p, jc, jb, :, core] + other[p, jc, jb] + in_c[p, r]
            else:
                held[p, jc, jb] = part_ref[p, jc, jb, :, core] + other[p, jc, jb]
            slot = (4 if up else 8) + r
            push(held.at[p, jc, jb], in_c.at[p, slot], moved(xyz, c, by), core, rc.at[p, slot], sc.at[p, slot])
    def finish_c(r):
        for p, a, b, c, ia, ib, ic in info:
            jc, jb = ic, rel(ib, r)
            ready(p, 0, r, jc, jb)
            arrive(in_c.at[p, 4 + r], rc.at[p, 4 + r])
            arrive(in_c.at[p, 8 + r], rc.at[p, 8 + r])
            held[p, jc, jb] = part_ref[p, jc, jb, :, core] + other[p, jc, jb] + (in_c[p, 4 + r] + in_c[p, 8 + r])
    def send_b(p, b, jc, jb, ja, slot, by):
        push(held.at[p, jc, jb, ja], in_b.at[p, slot], moved(xyz, b, by), core, rb.at[p, slot], sb.at[p, slot])
    finish_c(2)
    for q in FIRST:
        for p, a, b, c, ia, ib, ic in info:
            send_b(p, b, ic, rel(ib, 2), rel(ia, q), q, 1 if q in UP else -1)
    finish_c(3)
    finish_c(1)
    for q in (3, 0):
        for p, a, b, c, ia, ib, ic in info:
            send_b(p, b, ic, rel(ib, 1), rel(ia, q), 4 + q, 1)
    for q in (2, 1):
        for p, a, b, c, ia, ib, ic in info:
            send_b(p, b, ic, rel(ib, 3), rel(ia, q), 8 + q, -1)
    for up, q in ((True, 2), (False, 3), (True, 1), (False, 0)):
        for p, a, b, c, ia, ib, ic in info:
            by = 1 if up else -1
            jc, jb, ja = ic, rel(ib, by), rel(ia, q)
            arrive(in_b.at[p, q], rb.at[p, q])
            held[p, jc, jb, ja] = held[p, jc, jb, ja] + in_b[p, q]
            send_b(p, b, jc, jb, ja, (4 if up else 8) + q, by)
    finish_c(0)
    def finish_b(q):
        for p, a, b, c, ia, ib, ic in info:
            ja = rel(ia, q)
            arrive(in_b.at[p, 4 + q], rb.at[p, 4 + q])
            arrive(in_b.at[p, 8 + q], rb.at[p, 8 + q])
            held[p, ic, ib, ja] = held[p, ic, ib, ja] + (in_b[p, 4 + q] + in_b[p, 8 + q])
    finish_b(2)
    lo, hi = pl.ds(0, 8), pl.ds(8, 8)
    for p, a, b, c, ia, ib, ic in info:
        blk = held.at[p, ic, ib, rel(ia, 2)]
        push(blk.at[lo], far_a.at[p, 0], moved(xyz, a, 1), core, ra.at[p, 0], sa.at[p, 0])
        push(blk.at[hi], far_a.at[p, 1], moved(xyz, a, -1), core, ra.at[p, 1], sa.at[p, 1])
    finish_b(1)
    finish_b(3)
    for p, a, b, c, ia, ib, ic in info:
        ja = rel(ia, 1)
        arrive(far_a.at[p, 0], ra.at[p, 0])
        held[p, ic, ib, ja, 0:8] = held[p, ic, ib, ja, 0:8] + far_a[p, 0]
        push(held.at[p, ic, ib, ja], in_a.at[p, 0], moved(xyz, a, 1), core, ra.at[p, 2], sa.at[p, 2])
        ja = rel(ia, 3)
        arrive(far_a.at[p, 1], ra.at[p, 1])
        held[p, ic, ib, ja, 8:16] = held[p, ic, ib, ja, 8:16] + far_a[p, 1]
        push(held.at[p, ic, ib, ja], in_a.at[p, 1], moved(xyz, a, -1), core, ra.at[p, 3], sa.at[p, 3])
    finish_b(0)
    for p, a, b, c, ia, ib, ic in info:
        arrive(in_a.at[p, 0], ra.at[p, 2])
        arrive(in_a.at[p, 1], ra.at[p, 3])
        out_ref[p] = held[p, ic, ib, ia] + (in_a[p, 0] + in_a[p, 1])
    for cp in pend:
        cp.wait_send()

def reduce_scatter(part):
    clusters, nodes = part.shape[-2:]
    D = pltpu.SemaphoreType.DMA
    V = lambda *s: pltpu.VMEM(s + (clusters, nodes), jnp.float32)
    return pl.pallas_call(
        scatter_body,
        out_shape=jax.ShapeDtypeStruct((3, clusters, nodes), jnp.float32),
        in_specs=[pl.BlockSpec(memory_space=pltpu.VMEM)],
        out_specs=pl.BlockSpec(memory_space=pltpu.VMEM),
        scratch_shapes=[V(3, 4, 4, 4), V(3, 4, 4, 4), V(3, 12, 4), V(3, 12),
                        pltpu.VMEM((3, 2, clusters // 2, nodes), jnp.float32), V(3, 2),
                        D((3, 16)), D((3, 16)), D((3, 12)), D((3, 12)), D((3, 12)), D((3, 12)),
                        D((3, 4)), D((3, 4))],
        compiler_params=pltpu.CompilerParams(collective_id=1, has_side_effects=True, vmem_limit_bytes=24 * 2**20),
        name="torus_scatter",
    )(part)

ROWS = 32
GROUP = 4
BATCH = 8

def pieces(value):
    high = value.astype(jnp.bfloat16)
    rest = value - high.astype(jnp.float32)
    mid = rest.astype(jnp.bfloat16)
    low = (rest - mid.astype(jnp.float32)).astype(jnp.bfloat16)
    return high, mid, low


def coeff_body(disp_ref, coords_ref, inverse_ref, table_ref):
    nodes = inverse_ref.shape[-1]
    for u in range(GROUP):
        c = pl.program_id(0) * GROUP + u
        left = jnp.concatenate([disp_ref[i, pl.ds(c, 1), :] for i in range(3)] + [jnp.zeros((5, nodes), jnp.float32)], axis=0)
        lh = left.astype(jnp.bfloat16)
        ll = (left - lh.astype(jnp.float32)).astype(jnp.bfloat16)
        both = jnp.concatenate([lh, ll], axis=0)
        whole = inverse_ref[u]
        ih = whole.astype(jnp.bfloat16)
        il = (whole - ih.astype(jnp.float32)).astype(jnp.bfloat16)
        top = jnp.dot(both, ih, preferred_element_type=jnp.float32)
        low = jnp.dot(both, il, preferred_element_type=jnp.float32)
        res = top[0:8] + (top[8:16] + low[0:8])
        for i in range(6):
            row = coords_ref[i, pl.ds(c, 1), :] if i < 3 else res[i - 3:i - 2]
            for q in range(4):
                table_ref[i // 2, c, pl.ds((i % 2) * 4 + q, 1), :] = row[:, q * 128:(q + 1) * 128]


def own_table(node_disp, node_coords, inverse):
    clusters, nodes = inverse.shape[0], inverse.shape[1]
    whole = pl.BlockSpec((3, clusters, nodes), lambda c: (0, 0, 0))
    return pl.pallas_call(
        coeff_body,
        grid=(clusters // GROUP,),
        out_shape=jax.ShapeDtypeStruct((3, clusters, 8, 128), jnp.float32),
        in_specs=[whole, whole, pl.BlockSpec((GROUP, nodes, nodes), lambda c: (c, 0, 0))],
        out_specs=pl.BlockSpec(memory_space=pltpu.VMEM),
        compiler_params=pltpu.CompilerParams(vmem_limit_bytes=24 * 2**20),
        name="coefficients",
    )(node_disp, node_coords, inverse)


def pairs_body(flat, pts_ref, frc_ref, lev_ref, table_ref, disp_ref, part_ref,
               rows, spots, raw, packed, mark, wide_a, wide_b, sums_a, sums_b, spread_all, tally, jobs, count, sem2):
    slots, tiles = flat.shape[1:]
    points = pts_ref.shape[-1]
    total = tiles * slots

    def fetch(t, carry):
        for k in range(slots):
            for p in range(3):
                rows[p, pl.ds(pl.multiple_of((t * slots + k) * 8, 8), 8), :] = table_ref[p, pl.ds(pl.multiple_of(flat[p, k, t] * 8, 8), 8), :]
        return carry
    lax.fori_loop(0, tiles, fetch, 0)

    def clear(g, carry):
        part_ref[0, pl.ds(pl.multiple_of(g * 16, 16), 16), :] = jnp.zeros((16, part_ref.shape[2]), jnp.float32)
        part_ref[1, pl.ds(pl.multiple_of(g * 16, 16), 16), :] = jnp.zeros((16, part_ref.shape[2]), jnp.float32)
        part_ref[2, pl.ds(pl.multiple_of(g * 16, 16), 16), :] = jnp.zeros((16, part_ref.shape[2]), jnp.float32)
        return carry
    lax.fori_loop(0, part_ref.shape[1] // 16, clear, 0)
    disp_ref[...] = jnp.zeros(disp_ref.shape, jnp.float32)

    def columns(t, carry):
        level = lev_ref[t].astype(jnp.float32) + 1.0
        weight = level / jnp.sum(level, axis=0, keepdims=True)
        raw[t, 6:14, :] = weight * 4.0
        raw[t, 14:16, :] = jnp.zeros((2, points), jnp.float32)
        for i in range(3):
            raw[t, i:i + 1, :] = pts_ref[i, pl.ds(t, 1), :]
            raw[t, 3 + i:4 + i, :] = frc_ref[i, pl.ds(t, 1), :]
        h, m, l = pieces(raw[t])
        packed[t, 0:16, :] = h
        packed[t, 16:32, :] = m
        packed[t, 32:48, :] = l
        return carry
    lax.fori_loop(0, tiles, columns, 0, unroll=2)

    def near(t, carry):
        dist = None
        for i in range(3):
            base = t * slots * 8 + (4 if i == 1 else 0)
            chunk = [rows[i // 2, pl.ds(base + r, slots, stride=8), :] for r in range(4)]
            low = jnp.minimum(jnp.minimum(chunk[0], chunk[1]), jnp.minimum(chunk[2], chunk[3]))
            high = jnp.maximum(jnp.maximum(chunk[0], chunk[1]), jnp.maximum(chunk[2], chunk[3]))
            low = jnp.min(low, axis=1, keepdims=True)
            high = jnp.max(high, axis=1, keepdims=True)
            at = pts_ref[i, pl.ds(t, 1), :]
            gap = jnp.maximum(jnp.maximum(low - at, at - high), 0.0)
            dist = gap * gap if dist is None else dist + gap * gap
        mark[pl.ds(pl.multiple_of(t * slots, slots), slots), :] = jnp.where(dist < 1.0001, 1.0, 0.0)
        return carry
    lax.fori_loop(0, tiles, near, 0, unroll=4)

    before = (lax.broadcasted_iota(jnp.int32, (points, points), 0) < lax.broadcasted_iota(jnp.int32, (points, points), 1))
    before = jnp.where(before, 1.0, 0.0).astype(jnp.bfloat16)
    flags = mark[...]
    ones = jnp.ones((16, points), jnp.bfloat16)
    fb = flags.astype(jnp.bfloat16)
    rank = jnp.dot(fb, before, preferred_element_type=jnp.float32)
    spots[...] = jnp.where(flags > 0.5, rank, -1.0)
    sums = lax.dot_general(ones, fb, (((1,), (1,)), ((), ())), preferred_element_type=jnp.float32)
    tally[...] = sums[0:8].astype(jnp.int32)
    cp = pltpu.make_async_copy(tally, count, sem2)
    cp.start()
    cp.wait()

    most = points // ROWS
    def list_pairs(h, m):
        for u in range(slots):
            q = h * slots + u
            for j in range(most):
                jobs[m + j] = q * 16 + j
            m = m + ((count[0, q] + (ROWS - 1)) >> 5)
        return m
    for u in range(BATCH):
        jobs[u] = most
    made = lax.fori_loop(0, tiles, list_pairs, BATCH)
    for u in range(4 * BATCH):
        jobs[made + u] = most
    trips = (made - BATCH + 2 * BATCH - 1) // (2 * BATCH)

    source = lax.broadcasted_iota(jnp.int32, (48, 6 * 128), 0) & 15
    spread = jnp.where(source == (lax.broadcasted_iota(jnp.int32, (48, 6 * 128), 1) >> 7), 1.0, 0.0).astype(jnp.bfloat16)
    spread_all[...] = spread
    every = jnp.ones((48, 128), jnp.bfloat16)
    lane48 = lax.broadcasted_iota(jnp.int32, (ROWS, 48), 1) & 15
    place32 = lax.broadcasted_iota(jnp.int32, (ROWS, points), 0).astype(jnp.float32)
    lane = lax.broadcasted_iota(jnp.int32, (ROWS, 128), 1)

    def pick_of(job):
        q, j = job >> 4, job & 15
        return q, jnp.where(place32 + (j * ROWS).astype(jnp.float32) == spots[pl.ds(q, 1), :], 1.0, 0.0).astype(jnp.bfloat16)

    def bring(batch, wide):
        plain, chosen = [], []
        for u in range(BATCH):
            q, pick = pick_of(jobs[(batch + 1) * BATCH + u])
            got = lax.dot_general(pick, packed[q // slots], (((1,), (1,)), ((), ())), preferred_element_type=jnp.float32)
            plain.append(got.astype(jnp.bfloat16))
            chosen.append(jnp.where(lane48 == 6 + q % slots, got, 0.0).astype(jnp.bfloat16))
        wide[:, 0:6 * 128] = jnp.dot(jnp.concatenate(plain, axis=0), spread_all[...], preferred_element_type=jnp.float32)
        wide[:, 6 * 128:7 * 128] = jnp.dot(jnp.concatenate(chosen, axis=0), every, preferred_element_type=jnp.float32)

    def work(batch, wide, sums):
        for slot in range(BATCH):
            q = jobs[(batch + 1) * BATCH + slot] >> 4
            px, py, pz, fx, fy, fz, weight = [wide[slot * ROWS:(slot + 1) * ROWS, i * 128:(i + 1) * 128] for i in range(7)]
            shown = [None] * 3
            loads = [[], [], []]
            for g in range(4):
                base = q * 8 + g
                dx = px - rows[0, pl.ds(base, 1), :]
                dy = py - rows[0, pl.ds(base + 4, 1), :]
                dz = pz - rows[1, pl.ds(base, 1), :]
                d2 = jnp.maximum(dx * dx + dy * dy + dz * dz, 1e-30)
                u = jnp.maximum(1.0 - d2 * lax.rsqrt(d2), 0.0)
                u2 = u * u
                val = ((u2 * u2) * weight) * (1.25 - u)
                for i, (pp, off) in enumerate(((1, 4), (2, 0), (2, 4))):
                    term = val * rows[pp, pl.ds(base + off, 1), :]
                    shown[i] = term if shown[i] is None else shown[i] + term
                for i, f in enumerate((fx, fy, fz)):
                    loads[i].append(jnp.sum(val * f, axis=0, keepdims=True))
            for i in range(3):
                sums[slot, i] = shown[i]
                part_ref[i, pl.ds(flat[i, q & 7, q >> 3], 1), :] += jnp.concatenate(loads[i], axis=1)

    def give(batch, sums):
        backs = []
        for slot in range(BATCH):
            q, pick = pick_of(jobs[(batch + 1) * BATCH + slot])
            cols = [jnp.sum(sums[slot, i], axis=1, keepdims=True) for i in range(3)]
            d = jnp.where(lane == 0, cols[0], jnp.where(lane == 1, cols[1], cols[2]))
            dt = jnp.transpose(d)[0:8]
            dh = dt.astype(jnp.bfloat16)
            dl = (dt - dh.astype(jnp.float32)).astype(jnp.bfloat16)
            back = jnp.dot(jnp.concatenate([dh, dl], axis=0), pick, preferred_element_type=jnp.float32)
            backs.append((q // slots, back[0:8] + back[8:16]))
        for t, back in backs:
            for i in range(3):
                disp_ref[i, pl.ds(t, 1), :] += back[i:i + 1]

    sums_b[...] = jnp.zeros(sums_b.shape, jnp.float32)
    bring(0, wide_a)

    def trip(n, carry):
        bring(2 * n + 1, wide_b)
        work(2 * n, wide_a, sums_a)
        give(2 * n - 1, sums_b)
        bring(2 * n + 2, wide_a)
        work(2 * n + 1, wide_b, sums_b)
        give(2 * n, sums_a)
        return carry
    lax.fori_loop(0, trips, trip, 0)
    give(2 * trips - 1, sums_b)


def pairs(flat, pts, frc, lev, table):
    slots, tiles = flat.shape[1:]
    points = pts.shape[-1]
    total = tiles * slots
    clusters = table.shape[1] // 8
    vm = pl.BlockSpec(memory_space=pltpu.VMEM)
    V = lambda s, d=jnp.float32: pltpu.VMEM(s, d)
    return pl.pallas_call(
        pairs_body,
        out_shape=(jax.ShapeDtypeStruct(pts.shape, jnp.float32), jax.ShapeDtypeStruct((3, clusters, 512), jnp.float32)),
        in_specs=[pl.BlockSpec(memory_space=pltpu.SMEM), vm, vm, vm, vm],
        out_specs=(vm, vm),
        scratch_shapes=[
            V((3, total * 8, 128)), V((total, points)), V((tiles, 16, points)), V((tiles, 48, points), jnp.bfloat16),
            V((total, points)), V((BATCH * ROWS, 7 * 128)), V((BATCH * ROWS, 7 * 128)),
            V((BATCH, 3, ROWS, 128)), V((BATCH, 3, ROWS, 128)),
            V((48, 6 * 128), jnp.bfloat16),
            V((8, total), jnp.int32),
            pltpu.SMEM((total * 8 + 5 * BATCH + 8,), jnp.int32), pltpu.SMEM((8, total), jnp.int32),
            pltpu.SemaphoreType.DMA,
        ],
        compiler_params=pltpu.CompilerParams(vmem_limit_bytes=16 * 2**20),
        name="pairs",
    )(flat, pts, frc, lev, table)


def homes(ids):
    l, dev = ids & 15, ids >> 4
    core, z, y, x = (dev >> 4) & 1, dev >> 5, dev & 3, (dev >> 2) & 3
    order = ((x, y, z), (y, z, x), (z, x, y))
    return jnp.stack([(((c * 4 + b) * 4 + a) * 2 + core) * 16 + l for a, b, c in order])


def on_device(point_coords, fluid_force, tile_clusters, pu_level, node_coords, node_disp, inverse):
    turn = lambda v: jnp.transpose(v, (1, 0, 2))
    table = all_gather(own_table(turn(node_disp), turn(node_coords), inverse))
    table = table.reshape(3, -1, 128)
    shown, part = pairs(homes(tile_clusters.T), turn(point_coords), turn(fluid_force), pu_level, table)
    force = reduce_scatter(part.reshape(3, 4, 4, 4, 2, node_coords.shape[0], node_coords.shape[2]))
    return turn(shown), turn(force)


def solution(mesh):
    spec = P(("row", "col"), None, None)
    return jax.shard_map(
        on_device,
        mesh=mesh,
        in_specs=(spec, spec, P(("row", "col"), None), spec, spec, spec, spec),
        out_specs=(spec, spec),
        check_vma=False,
    )
```

```python
import jax
import jax.numpy as jnp
from jax import lax
from jax.experimental import pallas as pl
from jax.experimental.pallas import tpu as pltpu
from jax.sharding import PartitionSpec as P

MESH = pl.DeviceIdType.MESH

def mod4(v):
    return lax.rem(v + 4, 4)

def place():
    row, col = lax.axis_index("row"), lax.axis_index("col")
    return [col // 4, lax.rem(col, 4), row // 2], lax.rem(row, 2)

def device(xyz, core):
    return (xyz[2] * 2 + core, xyz[0] * 4 + xyz[1])

def moved(xyz, dim, by):
    out = list(xyz)
    out[dim] = mod4(out[dim] + by)
    return out

def greet(xyz, core):
    barrier = pltpu.get_barrier_semaphore()
    for dim in range(3):
        for by in (1, -1):
            pl.semaphore_signal(barrier, inc=1, device_id=device(moved(xyz, dim, by), core), device_id_type=MESH)
    pl.semaphore_signal(barrier, inc=1, device_id=device(xyz, 1 - core), device_id_type=MESH)
    pl.semaphore_wait(barrier, 7)

ORDERS = ((0, 1, 2), (1, 2, 0), (2, 0, 1))

def gather_body(own_ref, out_ref, recv, send, near, sib_send, local):
    xyz, core = place()
    greet(xyz, core)
    half = own_ref.shape[1] // 2
    pend = []

    def push(src, dst, to, to_core, rsem, ssem):
        c = pltpu.make_async_remote_copy(src_ref=src, dst_ref=dst, send_sem=ssem, recv_sem=rsem,
                                         device_id=device(to, to_core), device_id_type=MESH)
        c.start()
        pend.append(c)

    def arrive(dst, rsem):
        pltpu.make_async_remote_copy(src_ref=dst, dst_ref=dst, send_sem=rsem, recv_sem=rsem,
                                     device_id=device(xyz, 1 - core), device_id_type=MESH).wait_recv()

    class Part:
        pass
    parts = []
    for p, (a, b, c) in enumerate(ORDERS):
        s = Part()
        s.p, s.a, s.b, s.c = p, a, b, c
        s.ia, s.ib, s.ic = xyz[a], xyz[b], xyz[c]
        s.nsend = 0
        parts.append(s)

    def block(s, ja, jb, jc, sub=None):
        r = out_ref.at[s.p, jc, jb, ja, core]
        return r if sub is None else r.at[sub]

    def group(s, jb, jc, k=None):
        return out_ref.at[s.p, jc, jb, :, core if k is None else k]

    def nsem(s):
        s.nsend += 1
        return send.at[s.p, s.nsend - 1]

    lo, hi = pl.ds(0, half), pl.ds(half, half)
    rel = lambda i, r: mod4(i + r)
    copies = []
    for s in parts:
        own = own_ref.at[s.p]
        cp = pltpu.make_async_copy(own, block(s, s.ia, s.ib, s.ic), local.at[s.p])
        cp.start()
        copies.append(cp)
        for d, by in ((0, 1), (1, -1)):
            push(own, block(s, s.ia, s.ib, s.ic), moved(xyz, s.a, by), core, recv.at[s.p, d], nsem(s))
    for s in parts:
        own = own_ref.at[s.p]
        for d, by in ((0, 1), (1, -1)):
            push(own, block(s, s.ia, s.ib, s.ic), moved(xyz, s.b, by), core, recv.at[s.p, 4 + 4 * d + 0], nsem(s))

    def send_b(s, r):
        ja = rel(s.ia, r)
        for d, by in ((0, 1), (1, -1)):
            push(block(s, ja, s.ib, s.ic), block(s, ja, s.ib, s.ic), moved(xyz, s.b, by), core,
                 recv.at[s.p, 4 + 4 * d + r], nsem(s))

    for s in parts:
        ja = rel(s.ia, -1)
        arrive(block(s, ja, s.ib, s.ic), recv.at[s.p, 0])
        push(block(s, ja, s.ib, s.ic, lo), block(s, ja, s.ib, s.ic, lo), moved(xyz, s.a, 1), core, recv.at[s.p, 2], nsem(s))
        ja2 = rel(s.ia, 1)
        arrive(block(s, ja2, s.ib, s.ic), recv.at[s.p, 1])
        push(block(s, ja2, s.ib, s.ic, hi), block(s, ja2, s.ib, s.ic, hi), moved(xyz, s.a, -1), core, recv.at[s.p, 3], nsem(s))
        send_b(s, 3)
        send_b(s, 1)

    def sib(s, jb, jc, slot):
        push(group(s, jb, jc), group(s, jb, jc), xyz, 1 - core, near.at[s.p, slot], sib_send.at[s.p, slot])

    def send_c(s, r):
        jb = rel(s.ib, r)
        for d, by in ((0, 1), (1, -1)):
            push(group(s, jb, s.ic), group(s, jb, s.ic), moved(xyz, s.c, by), core,
                 recv.at[s.p, 16 + 4 * d + r], nsem(s))
        sib(s, jb, s.ic, r)

    for s, cp in zip(parts, copies):
        ja = rel(s.ia, 2)
        arrive(block(s, ja, s.ib, s.ic, lo), recv.at[s.p, 2])
        arrive(block(s, ja, s.ib, s.ic, hi), recv.at[s.p, 3])
        send_b(s, 2)
        cp.wait()
        send_c(s, 0)
    for s in parts:
        for r in (0, 3, 1, 2):
            ja = rel(s.ia, r)
            for d, by in ((0, 1), (1, -1)):
                jb = rel(s.ib, -by)
                arrive(block(s, ja, jb, s.ic), recv.at[s.p, 4 + 4 * d + r])
                if (d == 0) == (r in (0, 3)):
                    push(block(s, ja, jb, s.ic), block(s, ja, jb, s.ic), moved(xyz, s.b, by), core,
                         recv.at[s.p, 12 + r], nsem(s))
        send_c(s, 3)
        send_c(s, 1)
    for s in parts:
        jb = rel(s.ib, 2)
        for r in (0, 3, 1, 2):
            arrive(block(s, rel(s.ia, r), jb, s.ic), recv.at[s.p, 12 + r])
        send_c(s, 2)
    for r in (0, 3, 1, 2):
        for s in parts:
            jb = rel(s.ib, r)
            for d, by in ((0, 1), (1, -1)):
                jc = rel(s.ic, -by)
                arrive(group(s, jb, jc), recv.at[s.p, 16 + 4 * d + r])
                if (d == 0) == (r in (0, 3)):
                    push(group(s, jb, jc), group(s, jb, jc), moved(xyz, s.c, by), core, recv.at[s.p, 24 + r], nsem(s))
                sib(s, jb, jc, 4 + 4 * d + r)
    for r in (0, 3, 1, 2):
        for s in parts:
            jb, jc = rel(s.ib, r), rel(s.ic, 2)
            arrive(group(s, jb, jc), recv.at[s.p, 24 + r])
            sib(s, jb, jc, 12 + r)
    for s in parts:
        for r in range(4):
            for slot, jc in ((r, s.ic), (4 + r, rel(s.ic, -1)), (8 + r, rel(s.ic, 1)), (12 + r, rel(s.ic, 2))):
                arrive(group(s, rel(s.ib, r), jc, 1 - core), near.at[s.p, slot])
    for c in pend:
        c.wait_send()

def all_gather(own):
    parts, clusters, rows, lanes = own.shape
    return pl.pallas_call(
        gather_body,
        out_shape=jax.ShapeDtypeStruct((parts, 4, 4, 4, 2, clusters, rows, lanes), jnp.float32),
        in_specs=[pl.BlockSpec(memory_space=pltpu.VMEM)],
        out_specs=pl.BlockSpec(memory_space=pltpu.VMEM),
        scratch_shapes=[
            pltpu.SemaphoreType.DMA((3, 28)),
            pltpu.SemaphoreType.DMA((3, 28)),
            pltpu.SemaphoreType.DMA((3, 16)),
            pltpu.SemaphoreType.DMA((3, 16)),
            pltpu.SemaphoreType.DMA((3,)),
        ],
        compiler_params=pltpu.CompilerParams(collective_id=0, has_side_effects=True, vmem_limit_bytes=2 * 2**20),
        name="torus_gather",
    )(own)


FIRST = (2, 3, 1, 0)
UP, DOWN = (2, 1), (3, 0)

def scatter_body(part_ref, out_ref, held, other, in_c, in_b, far_a, in_a,
                 near, near_send, rc, sc, rb, sb, ra, sa):
    xyz, core = place()
    pend = []
    rel = lambda i, r: mod4(i + r)
    info = []
    for p, (a, b, c) in enumerate(ORDERS):
        info.append((p, a, b, c, xyz[a], xyz[b], xyz[c]))

    def push(src, dst, to, to_core, rsem, ssem):
        cp = pltpu.make_async_remote_copy(src_ref=src, dst_ref=dst, send_sem=ssem, recv_sem=rsem,
                                          device_id=device(to, to_core), device_id_type=MESH)
        cp.start()
        pend.append(cp)

    def arrive(dst, rsem):
        pltpu.make_async_remote_copy(src_ref=dst, dst_ref=dst, send_sem=rsem, recv_sem=rsem,
                                     device_id=device(xyz, 1 - core), device_id_type=MESH).wait_recv()

    def swap(r4):
        for r in FIRST:
            for p, a, b, c, ia, ib, ic in info:
                jc, jb = rel(ic, r4), rel(ib, r)
                push(part_ref.at[p, jc, jb, :, 1 - core], other.at[p, jc, jb], xyz, 1 - core,
                     near.at[p, r4 * 4 + r], near_send.at[p, r4 * 4 + r])
    greet(xyz, core)
    for r4 in (2, 1, 3, 0):
        swap(r4)

    def ready(p, r4, r, jc, jb):
        arrive(other.at[p, jc, jb], near.at[p, r4 * 4 + r])

    for r in FIRST:
        for p, a, b, c, ia, ib, ic in info:
            jc, jb = rel(ic, 2), rel(ib, r)
            ready(p, 2, r, jc, jb)
            held[p, jc, jb] = part_ref[p, jc, jb, :, core] + other[p, jc, jb]
            push(held.at[p, jc, jb], in_c.at[p, r], moved(xyz, c, 1 if r in UP else -1), core, rc.at[p, r], sc.at[p, r])
    for up, r, far in ((True, 3, False), (False, 2, False), (True, 0, False), (False, 1, False),
                       (True, 2, True), (False, 3, True), (True, 1, True), (False, 0, True)):
        for p, a, b, c, ia, ib, ic in info:
            by = 1 if up else -1
            jc, jb = rel(ic, by), rel(ib, r)
            ready(p, 1 if up else 3, r, jc, jb)
            if far:
                arrive(in_c.at[p, r], rc.at[p, r])
                held[p, jc, jb] = part_ref[p, jc, jb, :, core] + other[p, jc, jb] + in_c[p, r]
            else:
                held[p, jc, jb] = part_ref[p, jc, jb, :, core] + other[p, jc, jb]
            slot = (4 if up else 8) + r
            push(held.at[p, jc, jb], in_c.at[p, slot], moved(xyz, c, by), core, rc.at[p, slot], sc.at[p, slot])
    def finish_c(r):
        for p, a, b, c, ia, ib, ic in info:
            jc, jb = ic, rel(ib, r)
            ready(p, 0, r, jc, jb)
            arrive(in_c.at[p, 4 + r], rc.at[p, 4 + r])
            arrive(in_c.at[p, 8 + r], rc.at[p, 8 + r])
            held[p, jc, jb] = part_ref[p, jc, jb, :, core] + other[p, jc, jb] + (in_c[p, 4 + r] + in_c[p, 8 + r])
    def send_b(p, b, jc, jb, ja, slot, by):
        push(held.at[p, jc, jb, ja], in_b.at[p, slot], moved(xyz, b, by), core, rb.at[p, slot], sb.at[p, slot])
    finish_c(2)
    for q in FIRST:
        for p, a, b, c, ia, ib, ic in info:
            send_b(p, b, ic, rel(ib, 2), rel(ia, q), q, 1 if q in UP else -1)
    finish_c(3)
    finish_c(1)
    for q in (3, 0):
        for p, a, b, c, ia, ib, ic in info:
            send_b(p, b, ic, rel(ib, 1), rel(ia, q), 4 + q, 1)
    for q in (2, 1):
        for p, a, b, c, ia, ib, ic in info:
            send_b(p, b, ic, rel(ib, 3), rel(ia, q), 8 + q, -1)
    for up, q in ((True, 2), (False, 3), (True, 1), (False, 0)):
        for p, a, b, c, ia, ib, ic in info:
            by = 1 if up else -1
            jc, jb, ja = ic, rel(ib, by), rel(ia, q)
            arrive(in_b.at[p, q], rb.at[p, q])
            held[p, jc, jb, ja] = held[p, jc, jb, ja] + in_b[p, q]
            send_b(p, b, jc, jb, ja, (4 if up else 8) + q, by)
    finish_c(0)
    def finish_b(q):
        for p, a, b, c, ia, ib, ic in info:
            ja = rel(ia, q)
            arrive(in_b.at[p, 4 + q], rb.at[p, 4 + q])
            arrive(in_b.at[p, 8 + q], rb.at[p, 8 + q])
            held[p, ic, ib, ja] = held[p, ic, ib, ja] + (in_b[p, 4 + q] + in_b[p, 8 + q])
    finish_b(2)
    lo, hi = pl.ds(0, 8), pl.ds(8, 8)
    for p, a, b, c, ia, ib, ic in info:
        blk = held.at[p, ic, ib, rel(ia, 2)]
        push(blk.at[lo], far_a.at[p, 0], moved(xyz, a, 1), core, ra.at[p, 0], sa.at[p, 0])
        push(blk.at[hi], far_a.at[p, 1], moved(xyz, a, -1), core, ra.at[p, 1], sa.at[p, 1])
    finish_b(1)
    finish_b(3)
    for p, a, b, c, ia, ib, ic in info:
        ja = rel(ia, 1)
        arrive(far_a.at[p, 0], ra.at[p, 0])
        held[p, ic, ib, ja, 0:8] = held[p, ic, ib, ja, 0:8] + far_a[p, 0]
        push(held.at[p, ic, ib, ja], in_a.at[p, 0], moved(xyz, a, 1), core, ra.at[p, 2], sa.at[p, 2])
        ja = rel(ia, 3)
        arrive(far_a.at[p, 1], ra.at[p, 1])
        held[p, ic, ib, ja, 8:16] = held[p, ic, ib, ja, 8:16] + far_a[p, 1]
        push(held.at[p, ic, ib, ja], in_a.at[p, 1], moved(xyz, a, -1), core, ra.at[p, 3], sa.at[p, 3])
    finish_b(0)
    for p, a, b, c, ia, ib, ic in info:
        arrive(in_a.at[p, 0], ra.at[p, 2])
        arrive(in_a.at[p, 1], ra.at[p, 3])
        out_ref[p] = held[p, ic, ib, ia] + (in_a[p, 0] + in_a[p, 1])
    for cp in pend:
        cp.wait_send()

def reduce_scatter(part):
    clusters, nodes = part.shape[-2:]
    D = pltpu.SemaphoreType.DMA
    V = lambda *s: pltpu.VMEM(s + (clusters, nodes), jnp.float32)
    return pl.pallas_call(
        scatter_body,
        out_shape=jax.ShapeDtypeStruct((3, clusters, nodes), jnp.float32),
        in_specs=[pl.BlockSpec(memory_space=pltpu.VMEM)],
        out_specs=pl.BlockSpec(memory_space=pltpu.VMEM),
        scratch_shapes=[V(3, 4, 4, 4), V(3, 4, 4, 4), V(3, 12, 4), V(3, 12),
                        pltpu.VMEM((3, 2, clusters // 2, nodes), jnp.float32), V(3, 2),
                        D((3, 16)), D((3, 16)), D((3, 12)), D((3, 12)), D((3, 12)), D((3, 12)),
                        D((3, 4)), D((3, 4))],
        compiler_params=pltpu.CompilerParams(collective_id=1, has_side_effects=True, vmem_limit_bytes=24 * 2**20),
        name="torus_scatter",
    )(part)

ROWS = 32
GROUP = 4
BATCH = 8

def pieces(value):
    high = value.astype(jnp.bfloat16)
    rest = value - high.astype(jnp.float32)
    mid = rest.astype(jnp.bfloat16)
    low = (rest - mid.astype(jnp.float32)).astype(jnp.bfloat16)
    return high, mid, low


def coeff_body(disp_ref, coords_ref, inverse_ref, table_ref):
    nodes = inverse_ref.shape[-1]
    for u in range(GROUP):
        c = pl.program_id(0) * GROUP + u
        left = jnp.concatenate([disp_ref[i, pl.ds(c, 1), :] for i in range(3)] + [jnp.zeros((5, nodes), jnp.float32)], axis=0)
        lh = left.astype(jnp.bfloat16)
        ll = (left - lh.astype(jnp.float32)).astype(jnp.bfloat16)
        both = jnp.concatenate([lh, ll], axis=0)
        whole = inverse_ref[u]
        ih = whole.astype(jnp.bfloat16)
        il = (whole - ih.astype(jnp.float32)).astype(jnp.bfloat16)
        top = jnp.dot(both, ih, preferred_element_type=jnp.float32)
        low = jnp.dot(both, il, preferred_element_type=jnp.float32)
        res = top[0:8] + (top[8:16] + low[0:8])
        for i in range(6):
            row = coords_ref[i, pl.ds(c, 1), :] if i < 3 else res[i - 3:i - 2]
            for q in range(4):
                table_ref[i // 2, c, pl.ds((i % 2) * 4 + q, 1), :] = row[:, q * 128:(q + 1) * 128]


def own_table(node_disp, node_coords, inverse):
    clusters, nodes = inverse.shape[0], inverse.shape[1]
    whole = pl.BlockSpec((3, clusters, nodes), lambda c: (0, 0, 0))
    return pl.pallas_call(
        coeff_body,
        grid=(clusters // GROUP,),
        out_shape=jax.ShapeDtypeStruct((3, clusters, 8, 128), jnp.float32),
        in_specs=[whole, whole, pl.BlockSpec((GROUP, nodes, nodes), lambda c: (c, 0, 0))],
        out_specs=pl.BlockSpec(memory_space=pltpu.VMEM),
        compiler_params=pltpu.CompilerParams(vmem_limit_bytes=56 * 2**20),
        name="coefficients",
    )(node_disp, node_coords, inverse)


def pairs_body(flat, pts_ref, frc_ref, lev_ref, table_ref, disp_ref, part_ref,
               rows, spots, raw, packed, mark, wide_a, wide_b, sums_a, sums_b, spread_all, tally, jobs, count, sem2):
    slots, tiles = flat.shape[1:]
    points = pts_ref.shape[-1]
    total = tiles * slots

    def fetch(t, carry):
        for k in range(slots):
            for p in range(3):
                rows[p, pl.ds(pl.multiple_of((t * slots + k) * 8, 8), 8), :] = table_ref[p, pl.ds(pl.multiple_of(flat[p, k, t] * 8, 8), 8), :]
        return carry
    lax.fori_loop(0, tiles, fetch, 0)

    def clear(g, carry):
        part_ref[0, pl.ds(pl.multiple_of(g * 16, 16), 16), :] = jnp.zeros((16, part_ref.shape[2]), jnp.float32)
        part_ref[1, pl.ds(pl.multiple_of(g * 16, 16), 16), :] = jnp.zeros((16, part_ref.shape[2]), jnp.float32)
        part_ref[2, pl.ds(pl.multiple_of(g * 16, 16), 16), :] = jnp.zeros((16, part_ref.shape[2]), jnp.float32)
        return carry
    lax.fori_loop(0, part_ref.shape[1] // 16, clear, 0)
    disp_ref[...] = jnp.zeros(disp_ref.shape, jnp.float32)

    def columns(t, carry):
        level = lev_ref[t].astype(jnp.float32) + 1.0
        weight = level / jnp.sum(level, axis=0, keepdims=True)
        raw[t, 6:14, :] = weight * 4.0
        raw[t, 14:16, :] = jnp.zeros((2, points), jnp.float32)
        for i in range(3):
            raw[t, i:i + 1, :] = pts_ref[i, pl.ds(t, 1), :]
            raw[t, 3 + i:4 + i, :] = frc_ref[i, pl.ds(t, 1), :]
        h, m, l = pieces(raw[t])
        packed[t, 0:16, :] = h
        packed[t, 16:32, :] = m
        packed[t, 32:48, :] = l
        return carry
    lax.fori_loop(0, tiles, columns, 0, unroll=2)

    def near(t, carry):
        dist = None
        for i in range(3):
            base = t * slots * 8 + (4 if i == 1 else 0)
            chunk = [rows[i // 2, pl.ds(base + r, slots, stride=8), :] for r in range(4)]
            low = jnp.minimum(jnp.minimum(chunk[0], chunk[1]), jnp.minimum(chunk[2], chunk[3]))
            high = jnp.maximum(jnp.maximum(chunk[0], chunk[1]), jnp.maximum(chunk[2], chunk[3]))
            low = jnp.min(low, axis=1, keepdims=True)
            high = jnp.max(high, axis=1, keepdims=True)
            at = pts_ref[i, pl.ds(t, 1), :]
            gap = jnp.maximum(jnp.maximum(low - at, at - high), 0.0)
            dist = gap * gap if dist is None else dist + gap * gap
        mark[pl.ds(pl.multiple_of(t * slots, slots), slots), :] = jnp.where(dist < 1.0001, 1.0, 0.0)
        return carry
    lax.fori_loop(0, tiles, near, 0, unroll=4)

    before = (lax.broadcasted_iota(jnp.int32, (points, points), 0) < lax.broadcasted_iota(jnp.int32, (points, points), 1))
    before = jnp.where(before, 1.0, 0.0).astype(jnp.bfloat16)
    flags = mark[...]
    ones = jnp.ones((16, points), jnp.bfloat16)
    fb = flags.astype(jnp.bfloat16)
    rank = jnp.dot(fb, before, preferred_element_type=jnp.float32)
    spots[...] = jnp.where(flags > 0.5, rank, -1.0)
    sums = lax.dot_general(ones, fb, (((1,), (1,)), ((), ())), preferred_element_type=jnp.float32)
    tally[...] = sums[0:8].astype(jnp.int32)
    cp = pltpu.make_async_copy(tally, count, sem2)
    cp.start()
    cp.wait()

    most = points // ROWS
    def list_pairs(h, m):
        for u in range(slots):
            q = h * slots + u
            for j in range(most):
                jobs[m + j] = q * 16 + j
            m = m + ((count[0, q] + (ROWS - 1)) >> 5)
        return m
    for u in range(BATCH):
        jobs[u] = most
    made = lax.fori_loop(0, tiles, list_pairs, BATCH)
    for u in range(4 * BATCH):
        jobs[made + u] = most
    trips = (made - BATCH + 2 * BATCH - 1) // (2 * BATCH)

    source = lax.broadcasted_iota(jnp.int32, (48, 6 * 128), 0) & 15
    spread = jnp.where(source == (lax.broadcasted_iota(jnp.int32, (48, 6 * 128), 1) >> 7), 1.0, 0.0).astype(jnp.bfloat16)
    spread_all[...] = spread
    every = jnp.ones((48, 128), jnp.bfloat16)
    lane48 = lax.broadcasted_iota(jnp.int32, (ROWS, 48), 1) & 15
    place32 = lax.broadcasted_iota(jnp.int32, (ROWS, points), 0).astype(jnp.float32)
    lane = lax.broadcasted_iota(jnp.int32, (ROWS, 128), 1)

    def pick_of(job):
        q, j = job >> 4, job & 15
        return q, jnp.where(place32 + (j * ROWS).astype(jnp.float32) == spots[pl.ds(q, 1), :], 1.0, 0.0).astype(jnp.bfloat16)

    def bring(batch, wide):
        plain, chosen = [], []
        for u in range(BATCH):
            q, pick = pick_of(jobs[(batch + 1) * BATCH + u])
            got = lax.dot_general(pick, packed[q // slots], (((1,), (1,)), ((), ())), preferred_element_type=jnp.float32)
            plain.append(got.astype(jnp.bfloat16))
            chosen.append(jnp.where(lane48 == 6 + q % slots, got, 0.0).astype(jnp.bfloat16))
        wide[:, 0:6 * 128] = jnp.dot(jnp.concatenate(plain, axis=0), spread_all[...], preferred_element_type=jnp.float32)
        wide[:, 6 * 128:7 * 128] = jnp.dot(jnp.concatenate(chosen, axis=0), every, preferred_element_type=jnp.float32)

    def work(batch, wide, sums):
        for slot in range(BATCH):
            q = jobs[(batch + 1) * BATCH + slot] >> 4
            px, py, pz, fx, fy, fz, weight = [wide[slot * ROWS:(slot + 1) * ROWS, i * 128:(i + 1) * 128] for i in range(7)]
            shown = [None] * 3
            loads = [[], [], []]
            for g in range(4):
                base = q * 8 + g
                dx = px - rows[0, pl.ds(base, 1), :]
                dy = py - rows[0, pl.ds(base + 4, 1), :]
                dz = pz - rows[1, pl.ds(base, 1), :]
                d2 = jnp.maximum(dx * dx + dy * dy + dz * dz, 1e-30)
                u = jnp.maximum(1.0 - d2 * lax.rsqrt(d2), 0.0)
                u2 = u * u
                val = ((u2 * u2) * weight) * (1.25 - u)
                for i, (pp, off) in enumerate(((1, 4), (2, 0), (2, 4))):
                    term = val * rows[pp, pl.ds(base + off, 1), :]
                    shown[i] = term if shown[i] is None else shown[i] + term
                for i, f in enumerate((fx, fy, fz)):
                    loads[i].append(jnp.sum(val * f, axis=0, keepdims=True))
            for i in range(3):
                sums[slot, i] = shown[i]
                part_ref[i, pl.ds(flat[i, q & 7, q >> 3], 1), :] += jnp.concatenate(loads[i], axis=1)

    def give(batch, sums):
        backs = []
        for slot in range(BATCH):
            q, pick = pick_of(jobs[(batch + 1) * BATCH + slot])
            cols = [jnp.sum(sums[slot, i], axis=1, keepdims=True) for i in range(3)]
            d = jnp.where(lane == 0, cols[0], jnp.where(lane == 1, cols[1], cols[2]))
            dt = jnp.transpose(d)[0:8]
            dh = dt.astype(jnp.bfloat16)
            dl = (dt - dh.astype(jnp.float32)).astype(jnp.bfloat16)
            back = jnp.dot(jnp.concatenate([dh, dl], axis=0), pick, preferred_element_type=jnp.float32)
            backs.append((q // slots, back[0:8] + back[8:16]))
        for t, back in backs:
            for i in range(3):
                disp_ref[i, pl.ds(t, 1), :] += back[i:i + 1]

    sums_b[...] = jnp.zeros(sums_b.shape, jnp.float32)
    bring(0, wide_a)

    def trip(n, carry):
        bring(2 * n + 1, wide_b)
        work(2 * n, wide_a, sums_a)
        give(2 * n - 1, sums_b)
        bring(2 * n + 2, wide_a)
        work(2 * n + 1, wide_b, sums_b)
        give(2 * n, sums_a)
        return carry
    lax.fori_loop(0, trips, trip, 0)
    give(2 * trips - 1, sums_b)


def pairs(flat, pts, frc, lev, table):
    slots, tiles = flat.shape[1:]
    points = pts.shape[-1]
    total = tiles * slots
    clusters = table.shape[1] // 8
    vm = pl.BlockSpec(memory_space=pltpu.VMEM)
    V = lambda s, d=jnp.float32: pltpu.VMEM(s, d)
    return pl.pallas_call(
        pairs_body,
        out_shape=(jax.ShapeDtypeStruct(pts.shape, jnp.float32), jax.ShapeDtypeStruct((3, clusters, 512), jnp.float32)),
        in_specs=[pl.BlockSpec(memory_space=pltpu.SMEM), vm, vm, vm, vm],
        out_specs=(vm, vm),
        scratch_shapes=[
            V((3, total * 8, 128)), V((total, points)), V((tiles, 16, points)), V((tiles, 48, points), jnp.bfloat16),
            V((total, points)), V((BATCH * ROWS, 7 * 128)), V((BATCH * ROWS, 7 * 128)),
            V((BATCH, 3, ROWS, 128)), V((BATCH, 3, ROWS, 128)),
            V((48, 6 * 128), jnp.bfloat16),
            V((8, total), jnp.int32),
            pltpu.SMEM((total * 8 + 5 * BATCH + 8,), jnp.int32), pltpu.SMEM((8, total), jnp.int32),
            pltpu.SemaphoreType.DMA,
        ],
        compiler_params=pltpu.CompilerParams(vmem_limit_bytes=16 * 2**20),
        name="pairs",
    )(flat, pts, frc, lev, table)


def homes(ids):
    l, dev = ids & 15, ids >> 4
    core, z, y, x = (dev >> 4) & 1, dev >> 5, dev & 3, (dev >> 2) & 3
    order = ((x, y, z), (y, z, x), (z, x, y))
    return jnp.stack([(((c * 4 + b) * 4 + a) * 2 + core) * 16 + l for a, b, c in order])


def on_device(point_coords, fluid_force, tile_clusters, pu_level, node_coords, node_disp, inverse):
    turn = lambda v: jnp.transpose(v, (1, 0, 2))
    table = all_gather(own_table(turn(node_disp), turn(node_coords), inverse))
    table = table.reshape(3, -1, 128)
    shown, part = pairs(homes(tile_clusters.T), turn(point_coords), turn(fluid_force), pu_level, table)
    force = reduce_scatter(part.reshape(3, 4, 4, 4, 2, node_coords.shape[0], node_coords.shape[2]))
    return turn(shown), turn(force)


def solution(mesh):
    spec = P(("row", "col"), None, None)
    return jax.shard_map(
        on_device,
        mesh=mesh,
        in_specs=(spec, spec, P(("row", "col"), None), spec, spec, spec, spec),
        out_specs=(spec, spec),
        check_vma=False,
    )
```
